128 devices in a mesh: rep: 1, r: 16 (over y, z), s: 8 (over x, core).
Axes of the slice: x: 4, y: 4, z: 4, core: 2. Of those that a mesh axis runs over, the one named last changes fastest.
Arguments:
- x: bfloat16 [128, 2048, 1024], P(('rep', 'r', 's'))
- dy: bfloat16 [128, 2048, 1024], P(('rep', 'r', 's'))
- w_gate: bfloat16 [2, 1024, 3200], P(None, 's')
- w_up: bfloat16 [2, 1024, 3200], P(None, 's')
- w_down: bfloat16 [2, 3200, 1024], P(None, 's')
- m_w_gate: float32 [2, 1024, 3200], P(None, 's')
- m_w_up: float32 [2, 1024, 3200], P(None, 's')
- m_w_down: float32 [2, 3200, 1024], P(None, 's')
- v_w_gate: float32 [2, 1024, 3200], P(None, 's')
- v_w_up: float32 [2, 1024, 3200], P(None, 's')
- v_w_down: float32 [2, 3200, 1024], P(None, 's')
Outputs:
- output 1: bfloat16 [2, 1024, 3200], P('rep', 's')
- output 2: bfloat16 [2, 1024, 3200], P('rep', 's')
- output 3: bfloat16 [2, 3200, 1024], P('rep', 's')
- output 4: float32 [2, 1024, 3200], P('rep', 's')
- output 5: float32 [2, 1024, 3200], P('rep', 's')
- output 6: float32 [2, 3200, 1024], P('rep', 's')
- output 7: float32 [2, 1024, 3200], P('rep', 's')
- output 8: float32 [2, 1024, 3200], P('rep', 's')
- output 9: float32 [2, 3200, 1024], P('rep', 's')
All inputs are finite; a program needn't handle non-finite values.
Results may differ from the reference program's by a relative error of at most 0.022.
Values are sent between devices in bfloat16 or wider.
A program may use at most 1.5 GiB of HBM per device.

```python
import jax
import jax.numpy as jnp
from jax import lax

SEQUENCES = 128
TOKENS = 2048
D = 1024
FF = 3200
LAYERS = 2
NAMES = ("w_gate", "w_up", "w_down")
SHAPES = {"w_gate": (LAYERS, D, FF), "w_up": (LAYERS, D, FF), "w_down": (LAYERS, FF, D)}


def bump(key, n, height):
    away = (jnp.arange(n, dtype=jnp.int32) - jax.random.randint(key, (), 0, n, jnp.int32)) % n
    return jnp.where(away < n // 8, height, 1.0)


def together(key, own, strength):
    shared = jax.random.normal(key, own.shape[1:], jnp.float32)
    return (own + strength * shared) * lax.rsqrt(1 + strength * strength)


def setup_inputs(seed: int = 0, part: int = 0) -> dict:
    kx, kdy, ka, kb, kz, kf, kh, kl, *keys = jax.random.split(jax.random.key(seed), 8 + 3 * len(NAMES))
    kx, kdy, ka, kb = (jax.random.fold_in(k, part) for k in (kx, kdy, ka, kb))
    kw, km, kv = (keys[i::3] for i in range(3))
    shape = (SEQUENCES, TOKENS, D)
    much_x, much_dy = jax.random.uniform(kz, (2,), jnp.float32, 0.0, 1.0)
    loud = 2.0 ** jax.random.uniform(jax.random.fold_in(kz, 1), (), jnp.float32, -1.0, 2.0)
    layers = 2.0 ** jax.random.uniform(kl, (LAYERS, 1, 1), jnp.float32, -1.0, 1.0)
    x = together(ka, jax.random.normal(kx, shape, jnp.float32), much_x) * bump(kf, D, 4.0)
    dy = together(kb, jax.random.normal(kdy, shape, jnp.float32), much_dy)
    drawn = {"x": x.astype(jnp.bfloat16), "dy": (loud * dy * (SEQUENCES * TOKENS) ** -0.5).astype(jnp.bfloat16)}
    for key, name in zip(kw, NAMES, strict=True):
        w = jax.random.normal(key, SHAPES[name], jnp.float32) * SHAPES[name][1] ** -0.5
        drawn[name] = (w * {"w_gate": 1.0, "w_up": bump(kh, FF, 4.0), "w_down": layers}[name]).astype(jnp.bfloat16)
    for key, name in zip(km, NAMES, strict=True):
        drawn[f"m_{name}"] = 0.1 * jax.random.normal(key, SHAPES[name], jnp.float32)
    for key, name in zip(kv, NAMES, strict=True):
        drawn[f"v_{name}"] = loud * loud * jax.random.uniform(key, SHAPES[name], jnp.float32, 0.05, 0.15)
    return drawn


def matmul(a, w):
    return jnp.dot(a, w, preferred_element_type=jnp.float32).astype(jnp.bfloat16)


def normed(h):
    wide = h.astype(jnp.float32)
    scale = lax.rsqrt(jnp.mean(wide**2, -1, keepdims=True) + 1e-6)
    return (wide * scale).astype(jnp.bfloat16)


def layer(h, w):
    a = normed(h)
    gate = jnp.dot(a, w["w_gate"], preferred_element_type=jnp.float32)
    up = jnp.dot(a, w["w_up"], preferred_element_type=jnp.float32)
    return h + matmul((jax.nn.silu(gate) * up).astype(jnp.bfloat16), w["w_down"])


def adamw(w, m, v, g):
    m = 0.9 * m + 0.1 * g
    v = 0.95 * v + 0.05 * g * g
    step = m * lax.rsqrt(v + 1e-8) + 0.1 * w
    return (w - 0.02 * step).astype(jnp.bfloat16), m, v


def stack(weights, h):
    return lax.scan(lambda h, w: (layer(h, w), None), h, weights)[0]


def reference(x, dy, w_gate, w_up, w_down, m_w_gate, m_w_up, m_w_down, v_w_gate, v_w_up, v_w_down):
    weights = dict(zip(NAMES, (w_gate, w_up, w_down), strict=True))

    def take(so_far, sequence):
        h, by_y = sequence
        _, back = jax.vjp(lambda w: stack(w, h), weights)
        return jax.tree.map(lambda total, term: total + term.astype(jnp.float32), so_far, back(by_y)[0]), None

    none_yet = {name: jnp.zeros(w.shape, jnp.float32) for name, w in weights.items()}
    by_weights, _ = lax.scan(take, none_yet, (x, dy))
    gradients = [by_weights[name].astype(jnp.bfloat16).astype(jnp.float32) for name in NAMES]
    new = [
        adamw(w.astype(jnp.float32), m, v, g)
        for w, m, v, g in zip((w_gate, w_up, w_down), (m_w_gate, m_w_up, m_w_down), (v_w_gate, v_w_up, v_w_down), gradients, strict=True)
    ]
    return tuple(one[which] for which in range(3) for one in new)
```

```python
import functools

import jax
import jax.numpy as jnp
from jax import lax
from jax.experimental import pallas as pl
from jax.experimental.pallas import tpu as pltpu
from jax.sharding import PartitionSpec as P

BF, F32 = jnp.bfloat16, jnp.float32
MESH = pl.DeviceIdType.MESH
VMEM_LIMIT = 66_000_000
T, D, FF = 2048, 1024, 3200
TM = 512
CHUNKS = tuple((512 * j, 512) for j in range(6)) + ((3072, 128),)
GROUPS = ((0, 1024), (1024, 2176))
ANY = pl.BlockSpec(memory_space=pl.ANY)


def dot(a, b):
    return jnp.dot(a, b, preferred_element_type=F32)


def dot_bt(a, b):
    return lax.dot_general(a, b, (((1,), (1,)), ((), ())), preferred_element_type=F32)


def dot_at(a, b):
    return lax.dot_general(a, b, (((0,), (0,)), ((), ())), preferred_element_type=F32)


def normed(h):
    wide = h.astype(F32)
    scale = lax.rsqrt(jnp.mean(wide * wide, -1, keepdims=True) + 1e-6)
    return (wide * scale).astype(BF)


def cost(matmuls, nbytes):
    return pl.CostEstimate(flops=matmuls * 2 * T * D * FF, bytes_accessed=nbytes, transcendentals=0)


def forward_kernel(
    x_hbm, g_hbm, u_hbm, d_hbm,
    G, U, Dn, hid_hbm, a_hbm, h_hbm,
    x, stage_g, stage_u, stage_d, wg, wu, wd, hid, a_nat, a_t, hid_t,
    s1, r1, s2, r2, s3, r3, stage_sem, own_sem, x_sem, w_sem, hid_sem, a_sem, h_sem,
):
    r, s = lax.axis_index("r"), lax.axis_index("s")
    y, z = r // 4, r % 4
    cx, core = s // 2, s % 2

    def at_x(k):
        return {"r": r, "s": 2 * ((cx + k) % 4) + core}

    def at_y(k):
        return {"r": ((y + k) % 4) * 4 + z, "s": s}

    def at_z(k):
        return {"r": y * 4 + (z + k) % 4, "s": s}

    partner = {"r": r, "s": s + 1 - 2 * core}

    barrier = pltpu.get_barrier_semaphore()
    for to in [at(k) for at in (at_x, at_y, at_z) for k in (1, 2, 3)] + [partner]:
        pl.semaphore_signal(barrier, inc=1, device_id=to, device_id_type=MESH)
    pl.semaphore_wait(barrier, 10)

    mats = [m for l in range(2) for m in ((g_hbm, l, G, stage_g, 128), (u_hbm, l, U, stage_u, 128), (d_hbm, l, Dn, stage_d, 400))]

    def piece(rows, half, j):
        if rows == 128:
            return pl.ds(pl.multiple_of(half * 64 + j * 16, 16), 16), slice(None)
        return slice(None), pl.ds(pl.multiple_of(half * 512 + j * 128, 128), 128)

    def block(whole, l, b, rows, half=None, j=None):
        if half is None:
            return whole.at[l, b]
        p = piece(rows, half, j)
        return whole.at[l, b, p[0], p[1]]

    def c1(i, half, k):
        shard, l, whole, _, rows = mats[i]
        j = (y, z)[half]
        p = piece(rows, half, j)
        return pltpu.make_async_remote_copy(
            src_ref=shard.at[l, p[0], p[1]], dst_ref=block(whole, l, s, rows, half, j),
            send_sem=s1.at[i, half, k - 1], recv_sem=r1.at[i, half, k - 1], device_id=at_x(k), device_id_type=MESH)

    def c2(i, half, k, q):
        _, l, whole, _, rows = mats[i]
        b = 2 * ((cx + 4 - k) % 4) + core
        ref = block(whole, l, b, rows, half, (y, z)[half])
        return pltpu.make_async_remote_copy(
            src_ref=ref, dst_ref=ref, send_sem=s2.at[i, half, k - 1, q - 1], recv_sem=r2.at[i, half, k - 1, q - 1],
            device_id=(at_y, at_z)[half](q), device_id_type=MESH)

    def c3(i, k):
        shard, l, whole, _, rows = mats[i]
        b = 2 * ((cx + 4 - k) % 4) + core
        src = shard.at[l] if k == 0 else whole.at[l, b]
        return pltpu.make_async_remote_copy(
            src_ref=src, dst_ref=whole.at[l, b], send_sem=s3.at[i, k], recv_sem=r3.at[i, k], device_id=partner, device_id_type=MESH)

    def stage_in(i):
        shard, l, _, stage, _ = mats[i]
        return pltpu.make_async_copy(shard.at[l], stage.at[l], stage_sem.at[i])

    def stage_out(i):
        _, l, whole, stage, _ = mats[i]
        return pltpu.make_async_copy(stage.at[l], whole.at[l, s], own_sem.at[i])

    near_first = (1, 3, 2)

    def p1(i):
        for k in near_first:
            for half in range(2):
                c1(i, half, k).start()
        c3(i, 0).start()

    def p2(i):
        for k in near_first:
            for half in range(2):
                c1(i, half, k).wait_recv()
                for q in near_first:
                    c2(i, half, k, q).start()

    def p3(i):
        for k in near_first:
            for half in range(2):
                for q in near_first:
                    c2(i, half, k, q).wait_recv()
            c3(i, k).start()

    def arrived(i):
        for k in range(4):
            c3(i, k).wait_recv()

    loads = {0: wg, 1: wu, 2: wd}

    def load(i, b):
        _, l, whole, _, rows = mats[i]
        return pltpu.make_async_copy(whole.at[l, b], loads[i].at[pl.ds(b * rows, rows)], w_sem.at[i, b])

    def load_start(i):
        arrived(i)
        stage_out(i).wait()
        for b in range(8):
            load(i, b).start()

    def load_wait(i):
        for b in range(8):
            load(i, b).wait()

    for i in range(6):
        stage_in(i).start()
    for i in range(6):
        p1(i)
    x_copy = pltpu.make_async_copy(x_hbm, x, x_sem)
    x_copy.start()
    for i in range(6):
        stage_in(i).wait()
        stage_out(i).start()
    p2(0)
    p2(1)
    p3(0)
    p2(2)
    p2(3)
    load_start(0)
    p3(1)
    p2(4)
    load_start(1)
    x_copy.wait()
    load_wait(0)
    load_wait(1)

    def rows_of(m):
        return pl.ds(pl.multiple_of(m * TM, TM), TM)

    def hid_copy(m):
        return pltpu.make_async_copy(hid_t, hid_hbm.at[:, rows_of(m)], hid_sem.at[m])

    def a_copy(m):
        return pltpu.make_async_copy(a_t, a_hbm.at[:, rows_of(m)], a_sem.at[m])

    def h_copy(m):
        return pltpu.make_async_copy(x.at[rows_of(m)], h_hbm.at[rows_of(m)], h_sem.at[m])

    def up_step(m, carry):
        a = normed(x[rows_of(m), :])
        a_nat[...] = a

        @pl.when(m > 0)
        def _():
            a_copy(m - 1).wait()
            hid_copy(m - 1).wait()

        a_t[...] = a.T
        for start, size in CHUNKS:
            columns = pl.ds(start, size)
            gate, up = dot(a_nat[...], wg[:, columns]), dot(a_nat[...], wu[:, columns])
            one = (jax.nn.silu(gate) * up).astype(BF)
            hid[rows_of(m), columns] = one
            hid_t[columns, :] = one.T
        hid_copy(m).start()
        a_copy(m).start()

        @pl.when(m == 0)
        def _():
            p2(5)
            p3(2)

        @pl.when(m == 1)
        def _():
            p3(3)
            load_start(2)

        @pl.when(m == 2)
        def _():
            p3(4)

        return carry

    def down_step(m, carry):
        out = dot(hid[rows_of(m), :], wd[...]).astype(BF)
        x[rows_of(m), :] = (x[rows_of(m), :].astype(F32) + out.astype(F32)).astype(BF)
        h_copy(m).start()

        @pl.when(m == 1)
        def _():
            p3(5)

        return carry

    lax.fori_loop(0, 4, up_step, 0)
    load_wait(2)
    lax.fori_loop(0, 4, down_step, 0)

    for i in range(6):
        if i > 2:
            arrived(i)
            stage_out(i).wait()
        for k in (1, 2, 3):
            for half in range(2):
                c1(i, half, k).wait_send()
                for q in (1, 2, 3):
                    c2(i, half, k, q).wait_send()
        for k in range(4):
            c3(i, k).wait_send()
    hid_copy(3).wait()
    a_copy(3).wait()
    for m in range(4):
        h_copy(m).wait()


def forward(x, g, u, d):
    dma = pltpu.SemaphoreType.DMA
    return pl.pallas_call(
        forward_kernel,
        out_shape=(
            jax.ShapeDtypeStruct((2, 8, 128, FF), BF),
            jax.ShapeDtypeStruct((2, 8, 128, FF), BF),
            jax.ShapeDtypeStruct((2, 8, 400, D), BF),
            jax.ShapeDtypeStruct((FF, T), BF),
            jax.ShapeDtypeStruct((D, T), BF),
            jax.ShapeDtypeStruct((T, D), BF),
        ),
        in_specs=[ANY] * 4,
        out_specs=(ANY,) * 6,
        scratch_shapes=[
            pltpu.VMEM((T, D), BF),
            pltpu.VMEM((2, 128, FF), BF),
            pltpu.VMEM((2, 128, FF), BF),
            pltpu.VMEM((2, 400, D), BF),
            pltpu.VMEM((D, FF), BF),
            pltpu.VMEM((D, FF), BF),
            pltpu.VMEM((FF, D), BF),
            pltpu.VMEM((T, FF), BF),
            pltpu.VMEM((TM, D), BF),
            pltpu.VMEM((D, TM), BF),
            pltpu.VMEM((FF, TM), BF),
            dma((6, 2, 3)), dma((6, 2, 3)), dma((6, 2, 3, 3)), dma((6, 2, 3, 3)), dma((6, 4)), dma((6, 4)),
            dma((6,)), dma((6,)), dma, dma((3, 8)), dma((4,)), dma((4,)), dma((4,)),
        ],
        compiler_params=pltpu.CompilerParams(collective_id=0, has_side_effects=True, vmem_limit_bytes=VMEM_LIMIT),
        cost_estimate=cost(3, 60_000_000),
        name="forward",
    )(x, g, u, d)


def hidden_kernel(number, want_hid, h, by_y, G, U, Dn, *rest):
    outs, (a_nat, wg, wu, wd, sems) = rest[:-5], rest[-5:]
    hid_ref, a_ref = outs[:2] if want_hid else (None, None)
    dg_ref, du_ref = outs[-2:]
    m = pl.program_id(0)

    def copies(j):
        part = pl.ds(*GROUPS[j])
        return (
            pltpu.make_async_copy(G.at[number, :, part], wg.at[:, part], sems.at[0, j]),
            pltpu.make_async_copy(U.at[number, :, part], wu.at[:, part], sems.at[1, j]),
            pltpu.make_async_copy(Dn.at[number, part, :], wd.at[part, :], sems.at[2, j]),
        )

    @pl.when(m == 0)
    def _():
        for j in range(len(GROUPS)):
            for copy in copies(j):
                copy.start()

    a = normed(h[...])
    a_nat[...] = a
    if want_hid:
        a_ref[...] = a.T
    for j, (first, count) in enumerate(GROUPS):

        @pl.when(m == 0)
        def _():
            for copy in copies(j):
                copy.wait()

        for start, size in CHUNKS:
            if not first <= start < first + count:
                continue
            part = pl.ds(start, size)
            gate, up = dot(a_nat[...], wg[:, part]), dot(a_nat[...], wu[:, part])
            by_hid = dot_bt(by_y[...], wd[part, :]).astype(BF).astype(F32)
            sig = jax.nn.sigmoid(gate)
            act = gate * sig
            if want_hid:
                hid_ref[part, :] = (act * up).astype(BF).T
            du_ref[:, part] = (by_hid * act).astype(BF)
            dg_ref[:, part] = (by_hid * up * (sig + act * (1.0 - sig))).astype(BF)


def hidden(number, want_hid, h, by_y, G, U, Dn):
    tile = pl.BlockSpec((TM, D), lambda m: (m, 0))
    wide = pl.BlockSpec((TM, FF), lambda m: (m, 0))
    wide_shape = jax.ShapeDtypeStruct((T, FF), BF)
    extra_specs = (pl.BlockSpec((FF, TM), lambda m: (0, m)), pl.BlockSpec((D, TM), lambda m: (0, m))) if want_hid else ()
    extra_shapes = (jax.ShapeDtypeStruct((FF, T), BF), jax.ShapeDtypeStruct((D, T), BF)) if want_hid else ()
    return pl.pallas_call(
        functools.partial(hidden_kernel, number, want_hid),
        grid=(T // TM,),
        out_shape=extra_shapes + (wide_shape, wide_shape),
        in_specs=[tile, tile, ANY, ANY, ANY],
        out_specs=extra_specs + (wide, wide),
        scratch_shapes=[
            pltpu.VMEM((TM, D), BF),
            pltpu.VMEM((D, FF), BF),
            pltpu.VMEM((D, FF), BF),
            pltpu.VMEM((FF, D), BF),
            pltpu.SemaphoreType.DMA((3, len(GROUPS))),
        ],
        compiler_params=pltpu.CompilerParams(vmem_limit_bytes=VMEM_LIMIT, dimension_semantics=("arbitrary",)),
        cost_estimate=cost(3, 70_000_000),
        name=f"hidden_{number}",
    )(h, by_y, G.reshape(2, D, FF), U.reshape(2, D, FF), Dn.reshape(2, FF, D))


def input_kernel(number, h, by_y, dg, du, G, U, out, wg, wu, sems):
    m = pl.program_id(0)
    copies = [pltpu.make_async_copy(W.at[number], w, sems.at[i]) for i, (W, w) in enumerate(((G, wg), (U, wu)))]

    @pl.when(m == 0)
    def _():
        copies[0].start()
        copies[1].start()
        copies[0].wait()

    by_a = dot_bt(dg[...], wg[...]).astype(BF).astype(F32)

    @pl.when(m == 0)
    def _():
        copies[1].wait()

    by_a = (by_a + dot_bt(du[...], wu[...]).astype(BF).astype(F32)).astype(BF).astype(F32)
    wide = h[...].astype(F32)
    scale = lax.rsqrt(jnp.mean(wide * wide, -1, keepdims=True) + 1e-6)
    along = jnp.mean(by_a * wide, -1, keepdims=True)
    by_h = (by_a * scale - wide * (scale * scale * scale * along)).astype(BF)
    out[...] = (by_y[...].astype(F32) + by_h.astype(F32)).astype(BF)


def input_gradient(number, h, by_y, dg, du, G, U):
    tile = pl.BlockSpec((TM, D), lambda m: (m, 0))
    wide = pl.BlockSpec((TM, FF), lambda m: (m, 0))
    return pl.pallas_call(
        functools.partial(input_kernel, number),
        grid=(T // TM,),
        out_shape=jax.ShapeDtypeStruct((T, D), BF),
        in_specs=[tile, tile, wide, wide, ANY, ANY],
        out_specs=tile,
        scratch_shapes=[pltpu.VMEM((D, FF), BF), pltpu.VMEM((D, FF), BF), pltpu.SemaphoreType.DMA((2,))],
        compiler_params=pltpu.CompilerParams(vmem_limit_bytes=VMEM_LIMIT, dimension_semantics=("arbitrary",)),
        cost_estimate=cost(2, 50_000_000),
        name=f"input_{number}",
    )(h, by_y, dg, du, G.reshape(2, D, FF), U.reshape(2, D, FF))


UNITS = (
    ((64, 256), "yxz", "zy"),
    ((48, 256), "zxy", "yz"),
    ((16, 512), "xyz", "zy"),
    ((16, 512), "xzy", "yz"),
    ((16, 512), "yxz", "zy"),
    ((16, 512), "xzy", "yz"),
    ((16, 512), "xyz", "zy"),
    ((16, 512), "zxy", "yz"),
    ((16, 128), "xyz", "yz"),
)
NEAR_FIRST = (1, 3, 2)
KINDS = ((0, 1), (1, 1), (2, 6), (8, 1))


def gradients_kernel(
    aT, hidT, dg, du, by_y, g_out, u_out, d_out,
    a, rhs, rhs_tail, hid, send_d, send_e, send_u, send_t,
    *rest,
):
    bufs, (pair_s, pair_r, s, r, a_sem, rhs_sem, tail_sem, hid_sem, y_sem, out_sem) = rest[:32], rest[32:]
    ri, si = lax.axis_index("r"), lax.axis_index("s")
    core = si % 2
    me = {"x": si // 2, "y": ri // 4, "z": ri % 4}

    def peer(axis, k):
        if axis == "x":
            return {"r": ri, "s": 2 * ((me["x"] + k) % 4) + core}
        if axis == "y":
            return {"r": ((me["y"] + k) % 4) * 4 + me["z"], "s": si}
        return {"r": me["y"] * 4 + (me["z"] + k) % 4, "s": si}

    partner = {"r": ri, "s": si + 1 - 2 * core}
    barrier = pltpu.get_barrier_semaphore()
    for to in [peer(axis, k) for axis in "xyz" for k in (1, 2, 3)] + [partner]:
        pl.semaphore_signal(barrier, inc=1, device_id=to, device_id_type=MESH)
    pl.semaphore_wait(barrier, 10)

    def buffers(unit):
        for kind, (first, count) in enumerate(KINDS):
            if first <= unit < first + count:
                return [ref.at[unit - first] for ref in bufs[8 * kind : 8 * kind + 8]]

    def others(unit, stage):
        order = UNITS[unit][1]
        return [axis for axis in "xyz" if axis in order[stage:]]

    def cut(unit, stage, index):
        return tuple(index if axis == UNITS[unit][1][stage] else slice(None) for axis in others(unit, stage))

    def copies(unit, stage):
        P, R1, Q1, F1, R2, Q2, F2, RA = buffers(unit)
        order, gather = UNITS[unit][1:]
        made = []
        for k in NEAR_FIRST:
            if stage < 3:
                axis = order[stage]
                src = (P, Q1, Q2)[stage].at[cut(unit, stage, (me[axis] + k) % 4)]
                dst = (R1.at[k - 1], R2.at[k - 1], RA.at[0, k - 1])[stage]
            else:
                axis = gather[stage - 3]
                if stage == 3:
                    src = RA.at[1 + me["y"], me["z"]]
                elif axis == "y":
                    src = RA.at[1 + me["y"]]
                else:
                    src = RA.at[pl.ds(1, 4), me["z"]]
                dst = src
            made.append(pltpu.make_async_remote_copy(
                src_ref=src, dst_ref=dst, send_sem=s.at[unit, stage, k - 1], recv_sem=r.at[unit, stage, k - 1],
                device_id=peer(axis, k), device_id_type=MESH))
        return made

    def start(unit, stage):
        for copy in copies(unit, stage):
            copy.start()

    def wait(unit, stage):
        for copy in copies(unit, stage):
            copy.wait_recv()

    def out_copies(unit):
        RA = buffers(unit)[7]
        made = []
        if unit < 2:
            base, rows = 256 * unit, UNITS[unit][0][0]
            for y in range(4):
                for z in range(4 if unit == 0 else 3):
                    made.append((RA.at[1 + y, z], d_out.at[pl.ds(base + z * rows, rows), pl.ds(y * 256, 256)]))
        else:
            columns = pl.ds(*CHUNKS[unit - 2])
            for y in range(4):
                out = (g_out, u_out)[y // 2]
                made += [(RA.at[1 + y, z], out.at[pl.ds((y % 2) * 64 + z * 16, 16), columns]) for z in range(4)]
        return [pltpu.make_async_copy(src, dst, out_sem.at[unit, n]) for n, (src, dst) in enumerate(made)]

    def advance(unit, stage):
        P, R1, Q1, F1, R2, Q2, F2, RA = buffers(unit)
        wait(unit, stage)
        if stage < 3:
            axis = UNITS[unit][1][stage]
            mine = (P, F1, F2)[stage][cut(unit, stage, me[axis])].astype(F32)
            for k in range(3):
                mine += (R1[k] if stage == 0 else R2[k] if stage == 1 else RA[0, k]).astype(F32)
            if stage == 0:
                F1[...], Q1[...] = mine, mine.astype(BF)
            elif stage == 1:
                F2[...], Q2[...] = mine, mine.astype(BF)
            else:
                RA[1 + me["y"], me["z"]] = mine.astype(BF)
        if stage < 4:
            start(unit, stage + 1)
        else:
            for copy in out_copies(unit):
                copy.start()

    B, C, E, G1, G2 = range(5)
    after = {
        0: [("go", 2)],
        1: [("go", 3)],
        2: [("go", 4), (1, B)],
        3: [("go", 5), (2, B), (0, B), (1, C)],
        4: [("go", 6), (3, B), (2, C), (0, C), (1, E)],
        5: [("go", 7), (4, B), (5, B), (3, C), (2, E), (0, E), (1, G1)],
        6: [("go", 8), (4, C), (5, C), (3, E), (2, G1), (0, G1), (1, G2),
            (4, E), (5, E), (3, G1), (2, G2), (0, G2),
            (6, B), (7, B), (8, B), (4, G1), (5, G1), (3, G2),
            (6, C), (7, C), (8, C), (4, G2), (5, G2),
            (6, E), (7, E), (8, E), (6, G1), (7, G1), (8, G1), (6, G2), (7, G2), (8, G2)],
    }

    def run(tick):
        for what in after[tick]:
            if what[0] == "go":
                start(what[1], 0)
            else:
                advance(*what)

    def parity(half):
        return core if half else 1 - core

    def hid_copy(j):
        block = 2 * (j % 4) + jnp.where(j < 4, 1 - core, core)
        rows = pl.ds(pl.multiple_of(block * 400, 16), 400)
        return pltpu.make_async_copy(hidT.at[rows], hid.at[j % 2], hid_sem.at[j % 2])

    def y_copy(half):
        return pltpu.make_async_copy(by_y.at[:, pl.ds(half * 512, 512)], rhs.at[1, half], y_sem.at[half])

    def rhs_copy(n, mat):
        columns = pl.ds(pl.multiple_of(n * 512, 512), 512)
        return pltpu.make_async_copy((dg, du)[mat].at[:, columns], rhs.at[n % 2, mat], rhs_sem.at[n % 2, mat])

    def tail_copy(mat):
        return pltpu.make_async_copy((dg, du)[mat].at[:, pl.ds(3072, 128)], rhs_tail.at[mat], tail_sem.at[mat])

    PA, PB = buffers(0)[0], buffers(1)[0]

    def pair_d(k, which):
        src, dst = ((send_d, PA), (send_e, PB))[which]
        return pltpu.make_async_remote_copy(
            src_ref=src.at[k], dst_ref=dst.at[k], send_sem=pair_s.at[k, which], recv_sem=pair_r.at[k, which],
            device_id=partner, device_id_type=MESH)

    hid_copy(0).start()
    for half in range(2):
        y_copy(half).start()

    def a_copy(half, x):
        rows = pl.ds(pl.multiple_of((2 * x + parity(half)) * 128, 128), 128)
        return pltpu.make_async_copy(aT.at[rows], a.at[half, pl.ds(x * 128, 128)], a_sem.at[half, x])

    for half in range(2):
        for x in range(4):
            a_copy(half, x).start()
    for mat in range(2):
        rhs_copy(0, mat).start()
        tail_copy(mat).start()
    send_e[:, :, pl.ds(3, 1)] = jnp.zeros((4, 4, 1, 48, 256), BF)
    for half in range(2):
        y_copy(half).wait()

    def down_step(j, carry):
        hid_copy(j).wait()

        @pl.when(j < 7)
        def _():
            hid_copy(j + 1).start()

        k = j % 4
        for half in range(2):
            out = dot(hid[j % 2], rhs[1, half])
            upper = [out[:256, 256 * n : 256 * n + 256].reshape(4, 64, 256) for n in range(2)]
            lower = [out[256:, 256 * n : 256 * n + 256].reshape(3, 48, 256) for n in range(2)]
            if half == 0:

                @pl.when(j >= 4)
                def _():
                    pair_d(k, 0).wait_recv()
                    pair_d(k, 1).wait_recv()

            for n in range(2):
                y = 2 * half + n

                @pl.when(j < 4)
                def _():
                    send_d[k, y] = upper[n].astype(BF)
                    send_e[k, y, pl.ds(0, 3)] = lower[n].astype(BF)

                @pl.when(j >= 4)
                def _():
                    PA[k, y] = (PA[k, y].astype(F32) + upper[n]).astype(BF)
                    PB[k, y, pl.ds(0, 3)] = (PB[k, y, pl.ds(0, 3)].astype(F32) + lower[n]).astype(BF)

        @pl.when(j < 4)
        def _():
            pair_d(k, 0).start()
            pair_d(k, 1).start()

        return carry

    lax.fori_loop(0, 8, down_step, 0)
    for unit in range(2):
        start(unit, 0)
    for mat in range(2):
        rhs_copy(1, mat).start()
    for half in range(2):
        for x in range(4):
            a_copy(half, x).wait()

    def gate_up(P, send, rights, pair, columns):
        for mat in range(2):
            send[:, pl.ds(2 * mat, 2)] = dot(a[0], rights(mat)).astype(BF).reshape(4, 2, 4, 16, columns)
        pair.start()
        own = [dot(a[1], rights(mat)).reshape(4, 2, 4, 16, columns) for mat in range(2)]
        pair.wait_recv()
        for mat in range(2):
            part = pl.ds(2 * mat, 2)
            P[:, part] = (P[:, part].astype(F32) + own[mat]).astype(BF)

    def pair_u(n):
        return pltpu.make_async_remote_copy(
            src_ref=send_u.at[n % 2], dst_ref=bufs[16].at[n], send_sem=pair_s.at[4 + n, 0], recv_sem=pair_r.at[4 + n, 0],
            device_id=partner, device_id_type=MESH)

    pair_t = pltpu.make_async_remote_copy(
        src_ref=send_t, dst_ref=buffers(8)[0], send_sem=pair_s.at[10, 0], recv_sem=pair_r.at[10, 0],
        device_id=partner, device_id_type=MESH)

    def chunk_step(n, carry):
        for mat in range(2):
            rhs_copy(n, mat).wait()

        @pl.when(n >= 2)
        def _():
            pair_u(n - 2).wait_send()

        gate_up(bufs[16].at[n], send_u.at[n % 2], lambda mat: rhs[n % 2, mat], pair_u(n), 512)

        @pl.when(n < 4)
        def _():
            for mat in range(2):
                rhs_copy(n + 2, mat).start()

        for tick in range(6):

            @pl.when(n == tick)
            def _():
                run(tick)

        return carry

    lax.fori_loop(0, 6, chunk_step, 0)
    for mat in range(2):
        tail_copy(mat).wait()
    gate_up(buffers(8)[0], send_t, lambda mat: rhs_tail[mat], pair_t, 128)
    run(6)

    for k in range(4):
        for which in range(2):
            pair_d(k, which).wait_send()
    for n in (4, 5):
        pair_u(n).wait_send()
    pair_t.wait_send()
    for unit in range(len(UNITS)):
        for stage in range(5):
            for copy in copies(unit, stage):
                copy.wait_send()
        for copy in out_copies(unit):
            copy.wait()


def gradients(number, aT, hidT, dg, du, by_y):
    dma = pltpu.SemaphoreType.DMA
    bufs = []
    for first, count in KINDS:
        tile = UNITS[first][0]
        bufs += [
            pltpu.VMEM((count, 4, 4, 4) + tile, BF),
            pltpu.VMEM((count, 3, 4, 4) + tile, BF),
            pltpu.VMEM((count, 4, 4) + tile, BF),
            pltpu.VMEM((count, 4, 4) + tile, F32),
            pltpu.VMEM((count, 3, 4) + tile, BF),
            pltpu.VMEM((count, 4) + tile, BF),
            pltpu.VMEM((count, 4) + tile, F32),
            pltpu.VMEM((count, 5, 4) + tile, BF),
        ]
    return pl.pallas_call(
        gradients_kernel,
        out_shape=(
            jax.ShapeDtypeStruct((128, FF), BF),
            jax.ShapeDtypeStruct((128, FF), BF),
            jax.ShapeDtypeStruct((400, D), BF),
        ),
        in_specs=[ANY] * 5,
        out_specs=(ANY,) * 3,
        scratch_shapes=[
            pltpu.VMEM((2, 512, T), BF),
            pltpu.VMEM((2, 2, T, 512), BF),
            pltpu.VMEM((2, T, 128), BF),
            pltpu.VMEM((2, 400, T), BF),
            pltpu.VMEM((4, 4, 4, 64, 256), BF),
            pltpu.VMEM((4, 4, 4, 48, 256), BF),
            pltpu.VMEM((2, 4, 4, 4, 16, 512), BF),
            pltpu.VMEM((4, 4, 4, 16, 128), BF),
            *bufs,
            dma((11, 2)), dma((11, 2)), dma((9, 5, 3)), dma((9, 5, 3)), dma((2, 4)), dma((2, 2)), dma((2,)), dma((2,)), dma((2,)), dma((9, 16)),
        ],
        compiler_params=pltpu.CompilerParams(collective_id=1 + number, has_side_effects=True, vmem_limit_bytes=VMEM_LIMIT),
        cost_estimate=cost(3, 60_000_000),
        name=f"gradients_{number}",
    )(aT, hidT, dg, du, by_y)


def adamw(w, m, v, g):
    m = 0.9 * m + 0.1 * g
    v = 0.95 * v + 0.05 * g * g
    step = m * lax.rsqrt(v + 1e-8) + 0.1 * w
    return (w - 0.02 * step).astype(BF), m, v


def solution(mesh):
    def step(x, dy, *arrays):
        weights, m, v = (arrays[i : i + 3] for i in (0, 3, 6))
        x, dy = x[0], dy[0]
        G, U, Dn, hid0, a0, h1 = forward(x, *weights)
        hid1, a1, dg1, du1 = hidden(1, True, h1, dy, G, U, Dn)
        one = gradients(1, a1, hid1, dg1, du1, dy)
        by_h1 = input_gradient(1, h1, dy, dg1, du1, G, U)
        dg0, du0 = hidden(0, False, x, by_h1, G, U, Dn)
        zero = gradients(0, a0, hid0, dg0, du0, by_h1)
        summed = [jnp.stack(pair).astype(F32) for pair in zip(zero, one, strict=True)]
        new = [adamw(w.astype(F32), m, v, g) for w, m, v, g in zip(weights, m, v, summed, strict=True)]
        return tuple(one[which] for which in range(3) for one in new)

    states, cut = P(("rep", "r", "s"), None, None), P(None, "s", None)
    return jax.shard_map(
        step,
        mesh=mesh,
        in_specs=(states, states) + (cut,) * 9,
        out_specs=(P("rep", "s", None),) * 9,
        check_vma=False,
    )
```

```python
import functools

import jax
import jax.numpy as jnp
from jax import lax
from jax.experimental import pallas as pl
from jax.experimental.pallas import tpu as pltpu
from jax.sharding import PartitionSpec as P

BF, F32 = jnp.bfloat16, jnp.float32
MESH = pl.DeviceIdType.MESH
VMEM_LIMIT = 66_000_000
T, D, FF = 2048, 1024, 3200
WAY = 4
OWN = 400
TILE, LANES, SIDE, WIDE = 16, 128, 256, 512
TM = WIDE
CHUNKS = tuple((WIDE * j, WIDE) for j in range(6)) + ((3072, LANES),)
GROUPS = ((0, 1024), (1024, 2176))
ANY = pl.BlockSpec(memory_space=pl.ANY)


def dot(a, b):
    return jnp.dot(a, b, preferred_element_type=F32)


def dot_bt(a, b):
    return lax.dot_general(a, b, (((1,), (1,)), ((), ())), preferred_element_type=F32)


def dot_at(a, b):
    return lax.dot_general(a, b, (((0,), (0,)), ((), ())), preferred_element_type=F32)


def normed(h):
    wide = h.astype(F32)
    scale = lax.rsqrt(jnp.mean(wide * wide, -1, keepdims=True) + 1e-6)
    return (wide * scale).astype(BF)


def cost(matmuls, nbytes):
    return pl.CostEstimate(flops=matmuls * 2 * T * D * FF, bytes_accessed=nbytes, transcendentals=0)


def forward_kernel(
    x_hbm, g_hbm, u_hbm, d_hbm,
    G, U, Dn, hid_hbm, a_hbm, h_hbm,
    x, stage_g, stage_u, stage_d, wg, wu, wd, hid, a_nat, a_t, hid_t,
    s1, r1, s2, r2, s3, r3, stage_sem, own_sem, x_sem, w_sem, hid_sem, a_sem, h_sem,
):
    r, s = lax.axis_index("r"), lax.axis_index("s")
    y, z = r // WAY, r % WAY
    cx, core = s // 2, s % 2

    def at_x(k):
        return {"r": r, "s": 2 * ((cx + k) % WAY) + core}

    def at_y(k):
        return {"r": ((y + k) % WAY) * WAY + z, "s": s}

    def at_z(k):
        return {"r": y * WAY + (z + k) % WAY, "s": s}

    partner = {"r": r, "s": s + 1 - 2 * core}

    barrier = pltpu.get_barrier_semaphore()
    for to in [at(k) for at in (at_x, at_y, at_z) for k in (1, 2, 3)] + [partner]:
        pl.semaphore_signal(barrier, inc=1, device_id=to, device_id_type=MESH)
    pl.semaphore_wait(barrier, 10)

    mats = [m for l in range(2) for m in ((g_hbm, l, G, stage_g, LANES), (u_hbm, l, U, stage_u, LANES), (d_hbm, l, Dn, stage_d, OWN))]

    def piece(rows, half, j):
        if rows == LANES:
            return pl.ds(pl.multiple_of(half * 64 + j * TILE, TILE), TILE), slice(None)
        return slice(None), pl.ds(pl.multiple_of(half * WIDE + j * LANES, LANES), LANES)

    def block(whole, l, b, rows, half=None, j=None):
        if half is None:
            return whole.at[l, b]
        p = piece(rows, half, j)
        return whole.at[l, b, p[0], p[1]]

    def halved(ref, rows, back):
        if rows == LANES:
            return ref.at[:, pl.ds(1664 * back, 1664 - LANES * back)]
        return ref.at[pl.ds(208 * back, 208 - TILE * back), :]

    def source(k):
        return 2 * ((cx + WAY - k) % WAY) + core

    def c1(i, half, k):
        shard, l, whole, _, rows = mats[i]
        j = (y, z)[half]
        p = piece(rows, half, j)
        return pltpu.make_async_remote_copy(
            src_ref=shard.at[l, p[0], p[1]], dst_ref=block(whole, l, s, rows, half, j),
            send_sem=s1.at[i, half, k // 2], recv_sem=r1.at[i, half, k // 2], device_id=at_x(k), device_id_type=MESH)

    def f1(i, half, k):
        _, l, whole, _, rows = mats[i]
        ref = halved(block(whole, l, source(k), rows, half, (y, z)[half]), rows, k // 2)
        return pltpu.make_async_remote_copy(
            src_ref=ref, dst_ref=ref, send_sem=s1.at[i, half, 2 + k // 2], recv_sem=r1.at[i, half, 2 + k // 2],
            device_id=at_x(k), device_id_type=MESH)

    def c2(i, half, k, q):
        _, l, whole, _, rows = mats[i]
        ref = block(whole, l, source(k), rows, half, (y, z)[half])
        return pltpu.make_async_remote_copy(
            src_ref=ref, dst_ref=ref, send_sem=s2.at[i, half, k - 1, q // 2], recv_sem=r2.at[i, half, k - 1, q // 2],
            device_id=(at_y, at_z)[half](q), device_id_type=MESH)

    def f2(i, half, k, q):
        _, l, whole, _, rows = mats[i]
        ref = halved(block(whole, l, source(k), rows, half, ((y, z)[half] + WAY - q) % WAY), rows, q // 2)
        return pltpu.make_async_remote_copy(
            src_ref=ref, dst_ref=ref, send_sem=s2.at[i, half, k - 1, 2 + q // 2], recv_sem=r2.at[i, half, k - 1, 2 + q // 2],
            device_id=(at_y, at_z)[half](q), device_id_type=MESH)

    def c3(i, k):
        shard, l, whole, _, rows = mats[i]
        b = source(k)
        src = shard.at[l] if k == 0 else whole.at[l, b]
        return pltpu.make_async_remote_copy(
            src_ref=src, dst_ref=whole.at[l, b], send_sem=s3.at[i, k], recv_sem=r3.at[i, k], device_id=partner, device_id_type=MESH)

    def stage_in(i):
        shard, l, _, stage, _ = mats[i]
        return pltpu.make_async_copy(shard.at[l], stage.at[l], stage_sem.at[i])

    def stage_out(i):
        _, l, whole, stage, _ = mats[i]
        return pltpu.make_async_copy(stage.at[l], whole.at[l, s], own_sem.at[i])

    sides, halves = (1, 3), range(2)

    def p1(i):
        for k in sides:
            for half in halves:
                c1(i, half, k).start()
        c3(i, 0).start()

    def p2(i):
        for k in sides:
            for half in halves:
                c1(i, half, k).wait_recv()
                f1(i, half, k).start()
                for q in sides:
                    c2(i, half, k, q).start()

    def p2b(i):
        for half in halves:
            for k in sides:
                f1(i, half, k).wait_recv()
            for q in sides:
                c2(i, half, 2, q).start()
        for k in sides:
            for half in halves:
                for q in sides:
                    c2(i, half, k, q).wait_recv()
                    f2(i, half, k, q).start()

    def p2c(i):
        for half in halves:
            for q in sides:
                c2(i, half, 2, q).wait_recv()
                f2(i, half, 2, q).start()

    def p3(i):
        for k in (1, 3, 2):
            for half in halves:
                for q in sides:
                    f2(i, half, k, q).wait_recv()
            c3(i, k).start()

    def arrived(i):
        for k in range(WAY):
            c3(i, k).wait_recv()

    loads = {0: wg, 1: wu, 2: wd}

    def load(i, b):
        _, l, whole, _, rows = mats[i]
        return pltpu.make_async_copy(whole.at[l, b], loads[i].at[pl.ds(b * rows, rows)], w_sem.at[i, b])

    def load_start(i):
        arrived(i)
        stage_out(i).wait()
        for b in range(8):
            load(i, b).start()

    def load_wait(i):
        for b in range(8):
            load(i, b).wait()

    for i in range(6):
        stage_in(i).start()
    for i in range(6):
        p1(i)
    x_copy = pltpu.make_async_copy(x_hbm, x, x_sem)
    x_copy.start()
    for i in range(6):
        stage_in(i).wait()
        stage_out(i).start()
    p2(0)
    p2(1)
    p2b(0)
    p2c(0)
    p2(2)
    p2b(1)
    p3(0)
    p2c(1)
    p2(3)
    load_start(0)
    p2b(2)
    p3(1)
    p2c(2)
    p2(WAY)
    load_start(1)
    x_copy.wait()
    load_wait(0)
    load_wait(1)

    def rows_of(m):
        return pl.ds(pl.multiple_of(m * TM, TM), TM)

    def hid_copy(m):
        return pltpu.make_async_copy(hid_t, hid_hbm.at[:, rows_of(m)], hid_sem.at[m])

    def a_copy(m):
        return pltpu.make_async_copy(a_t, a_hbm.at[:, rows_of(m)], a_sem.at[m])

    def h_copy(m):
        return pltpu.make_async_copy(x.at[rows_of(m)], h_hbm.at[rows_of(m)], h_sem.at[m])

    def up_step(m, carry):
        a = normed(x[rows_of(m), :])
        a_nat[...] = a

        @pl.when(m > 0)
        def _():
            a_copy(m - 1).wait()
            hid_copy(m - 1).wait()

        a_t[...] = a.T
        for start, size in CHUNKS:
            columns = pl.ds(start, size)
            gate, up = dot(a_nat[...], wg[:, columns]), dot(a_nat[...], wu[:, columns])
            one = (jax.nn.silu(gate) * up).astype(BF)
            hid[rows_of(m), columns] = one
            hid_t[columns, :] = one.T
        hid_copy(m).start()
        a_copy(m).start()

        @pl.when(m == 0)
        def _():
            p2(5)
            p2b(3)
            p3(2)
            p2c(3)
            p2b(WAY)

        @pl.when(m == 1)
        def _():
            p3(3)
            load_start(2)
            p2c(WAY)
            p2b(5)

        @pl.when(m == 2)
        def _():
            p3(WAY)
            p2c(5)

        @pl.when(m == 3)
        def _():
            p3(5)

        return carry

    def down_step(m, carry):
        out = dot(hid[rows_of(m), :], wd[...]).astype(BF)
        x[rows_of(m), :] = (x[rows_of(m), :].astype(F32) + out.astype(F32)).astype(BF)
        h_copy(m).start()
        return carry

    lax.fori_loop(0, WAY, up_step, 0)
    load_wait(2)
    lax.fori_loop(0, WAY, down_step, 0)

    for i in range(6):
        if i > 2:
            arrived(i)
            stage_out(i).wait()
        for half in halves:
            for k in sides:
                c1(i, half, k).wait_send()
                f1(i, half, k).wait_send()
            for k in (1, 2, 3):
                for q in sides:
                    c2(i, half, k, q).wait_send()
                    f2(i, half, k, q).wait_send()
        for k in range(WAY):
            c3(i, k).wait_send()
    hid_copy(3).wait()
    a_copy(3).wait()
    for m in range(WAY):
        h_copy(m).wait()


def forward(x, g, u, d):
    dma = pltpu.SemaphoreType.DMA
    return pl.pallas_call(
        forward_kernel,
        out_shape=(
            jax.ShapeDtypeStruct((2, 8, LANES, FF), BF),
            jax.ShapeDtypeStruct((2, 8, LANES, FF), BF),
            jax.ShapeDtypeStruct((2, 8, OWN, D), BF),
            jax.ShapeDtypeStruct((FF, T), BF),
            jax.ShapeDtypeStruct((D, T), BF),
            jax.ShapeDtypeStruct((T, D), BF),
        ),
        in_specs=[ANY] * WAY,
        out_specs=(ANY,) * 6,
        scratch_shapes=[
            pltpu.VMEM((T, D), BF),
            pltpu.VMEM((2, LANES, FF), BF),
            pltpu.VMEM((2, LANES, FF), BF),
            pltpu.VMEM((2, OWN, D), BF),
            pltpu.VMEM((D, FF), BF),
            pltpu.VMEM((D, FF), BF),
            pltpu.VMEM((FF, D), BF),
            pltpu.VMEM((T, FF), BF),
            pltpu.VMEM((TM, D), BF),
            pltpu.VMEM((D, TM), BF),
            pltpu.VMEM((FF, TM), BF),
            dma((6, 2, WAY)), dma((6, 2, WAY)), dma((6, 2, 3, WAY)), dma((6, 2, 3, WAY)), dma((6, WAY)), dma((6, WAY)),
            dma((6,)), dma((6,)), dma, dma((3, 8)), dma((WAY,)), dma((WAY,)), dma((WAY,)),
        ],
        compiler_params=pltpu.CompilerParams(collective_id=0, has_side_effects=True, vmem_limit_bytes=VMEM_LIMIT),
        cost_estimate=cost(3, 60_000_000),
        name="forward",
    )(x, g, u, d)


def hidden_kernel(number, want_hid, h, by_y, G, U, Dn, *rest):
    outs, (a_nat, wg, wu, wd, sems) = rest[:-5], rest[-5:]
    hid_ref, a_ref = outs[:2] if want_hid else (None, None)
    dg_ref, du_ref = outs[-2:]
    m = pl.program_id(0)

    def copies(j):
        part = pl.ds(*GROUPS[j])
        return (
            pltpu.make_async_copy(G.at[number, :, part], wg.at[:, part], sems.at[0, j]),
            pltpu.make_async_copy(U.at[number, :, part], wu.at[:, part], sems.at[1, j]),
            pltpu.make_async_copy(Dn.at[number, part, :], wd.at[part, :], sems.at[2, j]),
        )

    @pl.when(m == 0)
    def _():
        for j in range(len(GROUPS)):
            for copy in copies(j):
                copy.start()

    a = normed(h[...])
    a_nat[...] = a
    if want_hid:
        a_ref[...] = a.T
    for j, (first, count) in enumerate(GROUPS):

        @pl.when(m == 0)
        def _():
            for copy in copies(j):
                copy.wait()

        for start, size in CHUNKS:
            if not first <= start < first + count:
                continue
            part = pl.ds(start, size)
            gate, up = dot(a_nat[...], wg[:, part]), dot(a_nat[...], wu[:, part])
            by_hid = dot_bt(by_y[...], wd[part, :]).astype(BF).astype(F32)
            sig = jax.nn.sigmoid(gate)
            act = gate * sig
            if want_hid:
                hid_ref[part, :] = (act * up).astype(BF).T
            du_ref[:, part] = (by_hid * act).astype(BF)
            dg_ref[:, part] = (by_hid * up * (sig + act * (1.0 - sig))).astype(BF)


def hidden(number, want_hid, h, by_y, G, U, Dn):
    tile = pl.BlockSpec((TM, D), lambda m: (m, 0))
    wide = pl.BlockSpec((TM, FF), lambda m: (m, 0))
    wide_shape = jax.ShapeDtypeStruct((T, FF), BF)
    extra_specs = (pl.BlockSpec((FF, TM), lambda m: (0, m)), pl.BlockSpec((D, TM), lambda m: (0, m))) if want_hid else ()
    extra_shapes = (jax.ShapeDtypeStruct((FF, T), BF), jax.ShapeDtypeStruct((D, T), BF)) if want_hid else ()
    return pl.pallas_call(
        functools.partial(hidden_kernel, number, want_hid),
        grid=(T // TM,),
        out_shape=extra_shapes + (wide_shape, wide_shape),
        in_specs=[tile, tile, ANY, ANY, ANY],
        out_specs=extra_specs + (wide, wide),
        scratch_shapes=[
            pltpu.VMEM((TM, D), BF),
            pltpu.VMEM((D, FF), BF),
            pltpu.VMEM((D, FF), BF),
            pltpu.VMEM((FF, D), BF),
            pltpu.SemaphoreType.DMA((3, len(GROUPS))),
        ],
        compiler_params=pltpu.CompilerParams(vmem_limit_bytes=VMEM_LIMIT, dimension_semantics=("arbitrary",)),
        cost_estimate=cost(3, 70_000_000),
        name=f"hidden_{number}",
    )(h, by_y, G.reshape(2, D, FF), U.reshape(2, D, FF), Dn.reshape(2, FF, D))


def input_kernel(number, h, by_y, dg, du, G, U, out, wg, wu, sems):
    m = pl.program_id(0)
    copies = [pltpu.make_async_copy(W.at[number], w, sems.at[i]) for i, (W, w) in enumerate(((G, wg), (U, wu)))]

    @pl.when(m == 0)
    def _():
        copies[0].start()
        copies[1].start()
        copies[0].wait()

    by_a = dot_bt(dg[...], wg[...]).astype(BF).astype(F32)

    @pl.when(m == 0)
    def _():
        copies[1].wait()

    by_a = (by_a + dot_bt(du[...], wu[...]).astype(BF).astype(F32)).astype(BF).astype(F32)
    wide = h[...].astype(F32)
    scale = lax.rsqrt(jnp.mean(wide * wide, -1, keepdims=True) + 1e-6)
    along = jnp.mean(by_a * wide, -1, keepdims=True)
    by_h = (by_a * scale - wide * (scale * scale * scale * along)).astype(BF)
    out[...] = (by_y[...].astype(F32) + by_h.astype(F32)).astype(BF)


def input_gradient(number, h, by_y, dg, du, G, U):
    tile = pl.BlockSpec((TM, D), lambda m: (m, 0))
    wide = pl.BlockSpec((TM, FF), lambda m: (m, 0))
    return pl.pallas_call(
        functools.partial(input_kernel, number),
        grid=(T // TM,),
        out_shape=jax.ShapeDtypeStruct((T, D), BF),
        in_specs=[tile, tile, wide, wide, ANY, ANY],
        out_specs=tile,
        scratch_shapes=[pltpu.VMEM((D, FF), BF), pltpu.VMEM((D, FF), BF), pltpu.SemaphoreType.DMA((2,))],
        compiler_params=pltpu.CompilerParams(vmem_limit_bytes=VMEM_LIMIT, dimension_semantics=("arbitrary",)),
        cost_estimate=cost(2, 50_000_000),
        name=f"input_{number}",
    )(h, by_y, dg, du, G.reshape(2, D, FF), U.reshape(2, D, FF))


UNITS = (
    ((64, SIDE), "yxz", "zy"),
    ((48, SIDE), "zxy", "yz"),
    ((TILE, WIDE), "xyz", "zy"),
    ((TILE, WIDE), "xzy", "yz"),
    ((TILE, WIDE), "yxz", "zy"),
    ((TILE, WIDE), "xzy", "yz"),
    ((TILE, WIDE), "xyz", "zy"),
    ((TILE, WIDE), "zxy", "yz"),
    ((TILE, LANES), "xyz", "yz"),
)
SIDES, NEAR_FIRST = (1, 3), (1, 3, 2)
KINDS = ((0, 1), (1, 1), (2, 6), (8, 1))


def gradients_kernel(
    aT, hidT, dg, du, by_y, g_out, u_out, d_out,
    a, rhs, rhs_tail, hid, send_d, send_e, send_u, send_t,
    *rest,
):
    bufs, (pair_s, pair_r, s, r, a_sem, rhs_sem, tail_sem, hid_sem, y_sem, out_sem) = rest[:32], rest[32:]
    ri, si = lax.axis_index("r"), lax.axis_index("s")
    core = si % 2
    me = {"x": si // 2, "y": ri // WAY, "z": ri % WAY}

    def peer(axis, k):
        if axis == "x":
            return {"r": ri, "s": 2 * ((me["x"] + k) % WAY) + core}
        if axis == "y":
            return {"r": ((me["y"] + k) % WAY) * WAY + me["z"], "s": si}
        return {"r": me["y"] * WAY + (me["z"] + k) % WAY, "s": si}

    partner = {"r": ri, "s": si + 1 - 2 * core}
    barrier = pltpu.get_barrier_semaphore()
    for to in [peer(axis, k) for axis in "xyz" for k in (1, 2, 3)] + [partner]:
        pl.semaphore_signal(barrier, inc=1, device_id=to, device_id_type=MESH)
    pl.semaphore_wait(barrier, 10)

    def buffers(unit):
        for kind, (first, count) in enumerate(KINDS):
            if first <= unit < first + count:
                return [ref.at[unit - first] for ref in bufs[8 * kind : 8 * kind + 8]]

    def others(unit, stage):
        order = UNITS[unit][1]
        return [axis for axis in "xyz" if axis in order[stage:]]

    def cut(unit, stage, index, half=None):
        axis, index_of = UNITS[unit][1][stage], []
        for one in others(unit, stage):
            if one == axis:
                index_of.append(index)
            elif half is None:
                index_of.append(slice(None))
            else:
                index_of.append(pl.ds(2 * half, 2))
                half = None
        return tuple(index_of)

    def halves_of(RA, axis, index, half=None):
        part = slice(None) if half is None else pl.ds(2 * half, 2)
        if axis == "y":
            return RA.at[1 + index, part]
        return RA.at[pl.ds(1, WAY) if half is None else pl.ds(1 + 2 * half, 2), index]

    def copies(unit, step):
        P, R1, Q1, F1, R2, Q2, F2, RA = buffers(unit)
        order, gather = UNITS[unit][1:]
        made = []
        for k in NEAR_FIRST if step in (WAY, 5) else SIDES:
            back = k // 2
            if step < WAY:
                stage = step // 2
                axis, src, dst = order[stage], (P, Q1)[stage], (R1, R2)[stage]
                if step % 2:
                    src, dst = src.at[cut(unit, stage, (me[axis] + k) % WAY)], dst.at[back]
                else:
                    src, dst = src.at[cut(unit, stage, (me[axis] + 2) % WAY, back)], dst.at[2, pl.ds(2 * back, 2)]
            elif step == WAY:
                axis = order[2]
                src, dst = Q2.at[(me[axis] + k) % WAY], RA.at[0, k - 1]
            elif step == 5:
                axis = gather[0]
                src = dst = RA.at[1 + me["y"], me["z"]]
            elif step == 6:
                axis = gather[1]
                src = dst = halves_of(RA, axis, me[axis])
            else:
                axis = gather[1]
                src = dst = halves_of(RA, axis, (me[axis] + WAY - k) % WAY, back)
            made.append(pltpu.make_async_remote_copy(
                src_ref=src, dst_ref=dst, send_sem=s.at[unit, step, k - 1], recv_sem=r.at[unit, step, k - 1],
                device_id=peer(axis, k), device_id_type=MESH))
        return made

    def start(unit, step):
        for copy in copies(unit, step):
            copy.start()

    def wait(unit, step):
        for copy in copies(unit, step):
            copy.wait_recv()

    def out_copies(unit):
        RA = buffers(unit)[7]
        made = []
        if unit < 2:
            base, rows = SIDE * unit, UNITS[unit][0][0]
            for y in range(WAY):
                for z in range(WAY if unit == 0 else 3):
                    made.append((RA.at[1 + y, z], d_out.at[pl.ds(base + z * rows, rows), pl.ds(y * SIDE, SIDE)]))
        else:
            columns = pl.ds(*CHUNKS[unit - 2])
            for y in range(WAY):
                out = (g_out, u_out)[y // 2]
                made += [(RA.at[1 + y, z], out.at[pl.ds((y % 2) * 64 + z * TILE, TILE), columns]) for z in range(WAY)]
        return [pltpu.make_async_copy(src, dst, out_sem.at[unit, n]) for n, (src, dst) in enumerate(made)]

    def advance(unit, step):
        P, R1, Q1, F1, R2, Q2, F2, RA = buffers(unit)
        wait(unit, step)
        stage = step // 2
        if step in (0, 2):
            axis, R, own, to = UNITS[unit][1][stage], (R1, R2)[stage], (P, F1)[stage], (P, Q1)[stage]
            for k in SIDES:
                index = cut(unit, stage, (me[axis] + k) % WAY, k // 2)
                to[index] = (own[index].astype(F32) + R[2, pl.ds(2 * (k // 2), 2)].astype(F32)).astype(BF)
        elif step in (1, 3):
            R, own, F, Q = (R1, R2)[stage], (P, F1)[stage], (F1, F2)[stage], (Q1, Q2)[stage]
            mine = own[cut(unit, stage, me[UNITS[unit][1][stage]])].astype(F32)
            mine += R[0].astype(F32) + R[1].astype(F32)
            F[...], Q[...] = mine, mine.astype(BF)
        elif step == WAY:
            mine = F2[me[UNITS[unit][1][2]]]
            for k in range(3):
                mine += RA[0, k].astype(F32)
            RA[1 + me["y"], me["z"]] = mine.astype(BF)
        if step < 7:
            start(unit, step + 1)
        else:
            for copy in out_copies(unit):
                copy.start()

    after = (
        ("cs",),
        ("dsb0a0c0",),
        ("esb1d0",),
        ("fsa1b2c1e0",),
        ("gsb3a2c2d1f0",),
        ("hsb4a3c3d2e1g0h0",),
        ("isb5a4c4d3e2f1i0", "b6a5c5d4e3f2b7a6c6d5e4f3a7c7", "d6e5f4g1h1i1d7e6f5g2h2i2e7f6", "g3h3i3f7g4h4i4g5h5i5g6h6i6g7h7i7"),
    )

    def run(tick):
        for what in after[tick]:
            for letter, step in zip(what[::2], what[1::2], strict=True):
                unit = ord(letter) - ord("a")
                if step == "s":
                    start(unit, 0)
                else:
                    advance(unit, int(step))

    def parity(half):
        return core if half else 1 - core

    def hid_copy(j):
        block = 2 * (j % WAY) + jnp.where(j < WAY, 1 - core, core)
        rows = pl.ds(pl.multiple_of(block * OWN, TILE), OWN)
        return pltpu.make_async_copy(hidT.at[rows], hid.at[j % 2], hid_sem.at[j % 2])

    def y_copy(half):
        return pltpu.make_async_copy(by_y.at[:, pl.ds(half * WIDE, WIDE)], rhs.at[1, half], y_sem.at[half])

    def rhs_copy(n, mat):
        columns = pl.ds(pl.multiple_of(n * WIDE, WIDE), WIDE)
        return pltpu.make_async_copy((dg, du)[mat].at[:, columns], rhs.at[n % 2, mat], rhs_sem.at[n % 2, mat])

    def tail_copy(mat):
        return pltpu.make_async_copy((dg, du)[mat].at[:, pl.ds(3072, LANES)], rhs_tail.at[mat], tail_sem.at[mat])

    PA, PB = buffers(0)[0], buffers(1)[0]

    def pair_d(k, which):
        src, dst = ((send_d, PA), (send_e, PB))[which]
        return pltpu.make_async_remote_copy(
            src_ref=src.at[k], dst_ref=dst.at[k], send_sem=pair_s.at[k, which], recv_sem=pair_r.at[k, which],
            device_id=partner, device_id_type=MESH)

    hid_copy(0).start()
    for half in range(2):
        y_copy(half).start()

    def a_copy(half, x):
        rows = pl.ds(pl.multiple_of((2 * x + parity(half)) * LANES, LANES), LANES)
        return pltpu.make_async_copy(aT.at[rows], a.at[half, pl.ds(x * LANES, LANES)], a_sem.at[half, x])

    for half in range(2):
        for x in range(WAY):
            a_copy(half, x).start()
    for mat in range(2):
        rhs_copy(0, mat).start()
        tail_copy(mat).start()
    send_e[:, :, pl.ds(3, 1)] = jnp.zeros((WAY, WAY, 1, 48, SIDE), BF)
    for half in range(2):
        y_copy(half).wait()

    def down_step(j, carry):
        hid_copy(j).wait()

        @pl.when(j < 7)
        def _():
            hid_copy(j + 1).start()

        k = j % WAY
        for half in range(2):
            out = dot(hid[j % 2], rhs[1, half])
            upper = [out[:SIDE, SIDE * n : SIDE * n + SIDE].reshape(WAY, 64, SIDE) for n in range(2)]
            lower = [out[SIDE:, SIDE * n : SIDE * n + SIDE].reshape(3, 48, SIDE) for n in range(2)]
            if half == 0:

                @pl.when(j >= WAY)
                def _():
                    pair_d(k, 0).wait_recv()
                    pair_d(k, 1).wait_recv()

            for n in range(2):
                y = 2 * half + n

                @pl.when(j < WAY)
                def _():
                    send_d[k, y] = upper[n].astype(BF)
                    send_e[k, y, pl.ds(0, 3)] = lower[n].astype(BF)

                @pl.when(j >= WAY)
                def _():
                    PA[k, y] = (PA[k, y].astype(F32) + upper[n]).astype(BF)
                    PB[k, y, pl.ds(0, 3)] = (PB[k, y, pl.ds(0, 3)].astype(F32) + lower[n]).astype(BF)

        @pl.when(j < WAY)
        def _():
            pair_d(k, 0).start()
            pair_d(k, 1).start()

        return carry

    lax.fori_loop(0, 8, down_step, 0)
    for unit in range(2):
        start(unit, 0)
    for mat in range(2):
        rhs_copy(1, mat).start()
    for half in range(2):
        for x in range(WAY):
            a_copy(half, x).wait()

    def gate_up(P, send, rights, pair, columns):
        for mat in range(2):
            send[:, pl.ds(2 * mat, 2)] = dot(a[0], rights(mat)).astype(BF).reshape(WAY, 2, WAY, TILE, columns)
        pair.start()
        own = [dot(a[1], rights(mat)).reshape(WAY, 2, WAY, TILE, columns) for mat in range(2)]
        pair.wait_recv()
        for mat in range(2):
            part = pl.ds(2 * mat, 2)
            P[:, part] = (P[:, part].astype(F32) + own[mat]).astype(BF)

    def pair_u(n):
        return pltpu.make_async_remote_copy(
            src_ref=send_u.at[n % 2], dst_ref=bufs[TILE].at[n], send_sem=pair_s.at[WAY + n, 0], recv_sem=pair_r.at[WAY + n, 0],
            device_id=partner, device_id_type=MESH)

    pair_t = pltpu.make_async_remote_copy(
        src_ref=send_t, dst_ref=buffers(8)[0], send_sem=pair_s.at[10, 0], recv_sem=pair_r.at[10, 0],
        device_id=partner, device_id_type=MESH)

    def chunk_step(n, carry):
        for mat in range(2):
            rhs_copy(n, mat).wait()

        @pl.when(n >= 2)
        def _():
            pair_u(n - 2).wait_send()

        gate_up(bufs[TILE].at[n], send_u.at[n % 2], lambda mat: rhs[n % 2, mat], pair_u(n), WIDE)

        @pl.when(n < WAY)
        def _():
            for mat in range(2):
                rhs_copy(n + 2, mat).start()

        for tick in range(6):

            @pl.when(n == tick)
            def _():
                run(tick)

        return carry

    lax.fori_loop(0, 6, chunk_step, 0)
    for mat in range(2):
        tail_copy(mat).wait()
    gate_up(buffers(8)[0], send_t, lambda mat: rhs_tail[mat], pair_t, LANES)
    run(6)

    for k in range(WAY):
        for which in range(2):
            pair_d(k, which).wait_send()
    for n in (WAY, 5):
        pair_u(n).wait_send()
    pair_t.wait_send()
    for unit in range(len(UNITS)):
        for step in range(8):
            for copy in copies(unit, step):
                copy.wait_send()
        for copy in out_copies(unit):
            copy.wait()


def gradients(number, aT, hidT, dg, du, by_y):
    dma = pltpu.SemaphoreType.DMA
    bufs = []
    for first, count in KINDS:
        tile = UNITS[first][0]
        bufs += [
            pltpu.VMEM((count, WAY, WAY, WAY) + tile, BF),
            pltpu.VMEM((count, 3, WAY, WAY) + tile, BF),
            pltpu.VMEM((count, WAY, WAY) + tile, BF),
            pltpu.VMEM((count, WAY, WAY) + tile, F32),
            pltpu.VMEM((count, 3, WAY) + tile, BF),
            pltpu.VMEM((count, WAY) + tile, BF),
            pltpu.VMEM((count, WAY) + tile, F32),
            pltpu.VMEM((count, 5, WAY) + tile, BF),
        ]
    return pl.pallas_call(
        gradients_kernel,
        out_shape=(
            jax.ShapeDtypeStruct((LANES, FF), BF),
            jax.ShapeDtypeStruct((LANES, FF), BF),
            jax.ShapeDtypeStruct((OWN, D), BF),
        ),
        in_specs=[ANY] * 5,
        out_specs=(ANY,) * 3,
        scratch_shapes=[
            pltpu.VMEM((2, WIDE, T), BF),
            pltpu.VMEM((2, 2, T, WIDE), BF),
            pltpu.VMEM((2, T, LANES), BF),
            pltpu.VMEM((2, OWN, T), BF),
            pltpu.VMEM((WAY, WAY, WAY, 64, SIDE), BF),
            pltpu.VMEM((WAY, WAY, WAY, 48, SIDE), BF),
            pltpu.VMEM((2, WAY, WAY, WAY, TILE, WIDE), BF),
            pltpu.VMEM((WAY, WAY, WAY, TILE, LANES), BF),
            *bufs,
            dma((11, 2)), dma((11, 2)), dma((9, 8, 3)), dma((9, 8, 3)), dma((2, WAY)), dma((2, 2)), dma((2,)), dma((2,)), dma((2,)), dma((9, TILE)),
        ],
        compiler_params=pltpu.CompilerParams(collective_id=1 + number, has_side_effects=True, vmem_limit_bytes=VMEM_LIMIT),
        cost_estimate=cost(3, 60_000_000),
        name=f"gradients_{number}",
    )(aT, hidT, dg, du, by_y)


def adamw(w, m, v, g):
    m = 0.9 * m + 0.1 * g
    v = 0.95 * v + 0.05 * g * g
    step = m * lax.rsqrt(v + 1e-8) + 0.1 * w
    return (w - 0.02 * step).astype(BF), m, v


def solution(mesh):
    def step(x, dy, *arrays):
        weights, m, v = (arrays[i : i + 3] for i in (0, 3, 6))
        x, dy = x[0], dy[0]
        G, U, Dn, hid0, a0, h1 = forward(x, *weights)
        hid1, a1, dg1, du1 = hidden(1, True, h1, dy, G, U, Dn)
        one = gradients(1, a1, hid1, dg1, du1, dy)
        by_h1 = input_gradient(1, h1, dy, dg1, du1, G, U)
        dg0, du0 = hidden(0, False, x, by_h1, G, U, Dn)
        zero = gradients(0, a0, hid0, dg0, du0, by_h1)
        summed = [jnp.stack(pair).astype(F32) for pair in zip(zero, one, strict=True)]
        new = [adamw(w.astype(F32), m, v, g) for w, m, v, g in zip(weights, m, v, summed, strict=True)]
        return tuple(one[which] for which in range(3) for one in new)

    states, cut = P(("rep", "r", "s"), None, None), P(None, "s", None)
    return jax.shard_map(
        step,
        mesh=mesh,
        in_specs=(states, states) + (cut,) * 9,
        out_specs=(P("rep", "s", None),) * 9,
        check_vma=False,
    )
```

```python
import functools

import jax
import jax.numpy as jnp
from jax import lax
from jax.experimental import pallas as pl
from jax.experimental.pallas import tpu as pltpu
from jax.sharding import PartitionSpec as P

BF, F32 = jnp.bfloat16, jnp.float32
MESH = pl.DeviceIdType.MESH
VMEM_LIMIT = 67_043_328
T, D, FF = 2048, 1024, 3200
WAY = 4
OWN = 400
TILE, LANES, SIDE, WIDE = 16, 128, 256, 512
TM = WIDE
CHUNKS = tuple((WIDE * j, WIDE) for j in range(6)) + ((3072, LANES),)
GROUPS = ((0, 1024), (1024, 2176))
ANY = pl.BlockSpec(memory_space=pl.ANY)
SIDES, NEAR_FIRST = (1, 3), (1, 3, 2)


def dot(a, b):
    return jnp.dot(a, b, preferred_element_type=F32)


def dot_bt(a, b):
    return lax.dot_general(a, b, (((1,), (1,)), ((), ())), preferred_element_type=F32)


def dot_at(a, b):
    return lax.dot_general(a, b, (((0,), (0,)), ((), ())), preferred_element_type=F32)


def normed(h):
    wide = h.astype(F32)
    scale = lax.rsqrt(jnp.mean(wide * wide, -1, keepdims=True) + 1e-6)
    return (wide * scale).astype(BF)


def cost(matmuls, nbytes):
    return pl.CostEstimate(flops=matmuls * 2 * T * D * FF, bytes_accessed=nbytes, transcendentals=0)


def forward_kernel(
    x_hbm, g_hbm, u_hbm, d_hbm,
    G, U, Dn, hid_hbm, a_hbm, h_hbm,
    x, stage_g, stage_u, stage_d, wg, wu, wd, hid, a_nat, a_t, hid_t,
    s1, r1, s2, r2, s3, r3, stage_sem, own_sem, x_sem, w_sem, hid_sem, a_sem, h_sem,
):
    r, s = lax.axis_index("r"), lax.axis_index("s")
    y, z = r // WAY, r % WAY
    cx, core = s // 2, s % 2

    def at_x(k):
        return {"r": r, "s": 2 * ((cx + k) % WAY) + core}

    def at_y(k):
        return {"r": ((y + k) % WAY) * WAY + z, "s": s}

    def at_z(k):
        return {"r": y * WAY + (z + k) % WAY, "s": s}

    partner = {"r": r, "s": s + 1 - 2 * core}

    barrier = pltpu.get_barrier_semaphore()
    for to in [at(k) for at in (at_x, at_y, at_z) for k in NEAR_FIRST] + [partner]:
        pl.semaphore_signal(barrier, inc=1, device_id=to, device_id_type=MESH)
    pl.semaphore_wait(barrier, 10)

    mats = [m for l in range(2) for m in ((g_hbm, l, G, stage_g, LANES), (u_hbm, l, U, stage_u, LANES), (d_hbm, l, Dn, stage_d, OWN))]

    def piece(rows, half, j):
        if rows == LANES:
            return pl.ds(pl.multiple_of(half * 64 + j * TILE, TILE), TILE), slice(None)
        return slice(None), pl.ds(pl.multiple_of(half * WIDE + j * LANES, LANES), LANES)

    def block(whole, l, b, rows, half=None, j=None):
        if half is None:
            return whole.at[l, b]
        p = piece(rows, half, j)
        return whole.at[l, b, p[0], p[1]]

    def c1(i, half, k):
        shard, l, whole, _, rows = mats[i]
        j = (y, z)[half]
        p = piece(rows, half, j)
        return pltpu.make_async_remote_copy(
            src_ref=shard.at[l, p[0], p[1]], dst_ref=block(whole, l, s, rows, half, j),
            send_sem=s1.at[i, half, k - 1], recv_sem=r1.at[i, half, k - 1], device_id=at_x(k), device_id_type=MESH)

    def c2(i, half, k, q):
        _, l, whole, _, rows = mats[i]
        b = 2 * ((cx + WAY - k) % WAY) + core
        ref = block(whole, l, b, rows, half, (y, z)[half])
        return pltpu.make_async_remote_copy(
            src_ref=ref, dst_ref=ref, send_sem=s2.at[i, half, k - 1, q - 1], recv_sem=r2.at[i, half, k - 1, q - 1],
            device_id=(at_y, at_z)[half](q), device_id_type=MESH)

    def c3(i, k):
        shard, l, whole, _, rows = mats[i]
        b = 2 * ((cx + WAY - k) % WAY) + core
        src = shard.at[l] if k == 0 else whole.at[l, b]
        return pltpu.make_async_remote_copy(
            src_ref=src, dst_ref=whole.at[l, b], send_sem=s3.at[i, k], recv_sem=r3.at[i, k], device_id=partner, device_id_type=MESH)

    def stage_in(i):
        shard, l, _, stage, _ = mats[i]
        return pltpu.make_async_copy(shard.at[l], stage.at[l], stage_sem.at[i])

    def stage_out(i):
        _, l, whole, stage, _ = mats[i]
        return pltpu.make_async_copy(stage.at[l], whole.at[l, s], own_sem.at[i])

    near_first = NEAR_FIRST

    def p1(i):
        for k in near_first:
            for half in range(2):
                c1(i, half, k).start()
        c3(i, 0).start()

    def p2(i):
        for k in near_first:
            for half in range(2):
                c1(i, half, k).wait_recv()
                for q in near_first:
                    c2(i, half, k, q).start()

    def p3(i):
        for k in near_first:
            for half in range(2):
                for q in near_first:
                    c2(i, half, k, q).wait_recv()
            c3(i, k).start()

    def arrived(i):
        for k in range(WAY):
            c3(i, k).wait_recv()

    loads = {0: wg, 1: wu, 2: wd}

    def load(i, b):
        _, l, whole, _, rows = mats[i]
        return pltpu.make_async_copy(whole.at[l, b], loads[i].at[pl.ds(b * rows, rows)], w_sem.at[i, b])

    def load_start(i):
        arrived(i)
        stage_out(i).wait()
        for b in range(8):
            load(i, b).start()

    def load_wait(i):
        for b in range(8):
            load(i, b).wait()

    for i in range(6):
        stage_in(i).start()
    for i in range(6):
        p1(i)
    x_copy = pltpu.make_async_copy(x_hbm, x, x_sem)
    x_copy.start()
    for i in range(6):
        stage_in(i).wait()
        stage_out(i).start()
    p2(0)
    p2(1)
    p3(0)
    p2(2)
    p2(3)
    load_start(0)
    p3(1)
    p2(WAY)
    load_start(1)
    x_copy.wait()
    load_wait(0)
    load_wait(1)

    def rows_of(m):
        return pl.ds(pl.multiple_of(m * TM, TM), TM)

    def hid_copy(m):
        return pltpu.make_async_copy(hid_t, hid_hbm.at[:, rows_of(m)], hid_sem.at[m])

    def a_copy(m):
        return pltpu.make_async_copy(a_t, a_hbm.at[:, rows_of(m)], a_sem.at[m])

    def h_copy(m):
        return pltpu.make_async_copy(x.at[rows_of(m)], h_hbm.at[rows_of(m)], h_sem.at[m])

    def up_step(m, carry):
        a = normed(x[rows_of(m), :])
        a_nat[...] = a

        @pl.when(m > 0)
        def _():
            a_copy(m - 1).wait()
            hid_copy(m - 1).wait()

        a_t[...] = a.T
        for start, size in CHUNKS:
            columns = pl.ds(start, size)
            gate, up = dot(a_nat[...], wg[:, columns]), dot(a_nat[...], wu[:, columns])
            one = (jax.nn.silu(gate) * up).astype(BF)
            hid[rows_of(m), columns] = one
            hid_t[columns, :] = one.T
        hid_copy(m).start()
        a_copy(m).start()

        @pl.when(m == 0)
        def _():
            p2(5)
            p3(2)

        @pl.when(m == 1)
        def _():
            p3(3)
            load_start(2)

        @pl.when(m == 2)
        def _():
            p3(WAY)

        return carry

    def down_step(m, carry):
        out = dot(hid[rows_of(m), :], wd[...]).astype(BF)
        x[rows_of(m), :] = (x[rows_of(m), :].astype(F32) + out.astype(F32)).astype(BF)
        h_copy(m).start()

        @pl.when(m == 1)
        def _():
            p3(5)

        return carry

    lax.fori_loop(0, WAY, up_step, 0)
    load_wait(2)
    lax.fori_loop(0, WAY, down_step, 0)

    for i in range(6):
        if i > 2:
            arrived(i)
            stage_out(i).wait()
        for k in NEAR_FIRST:
            for half in range(2):
                c1(i, half, k).wait_send()
                for q in NEAR_FIRST:
                    c2(i, half, k, q).wait_send()
        for k in range(WAY):
            c3(i, k).wait_send()
    hid_copy(3).wait()
    a_copy(3).wait()
    for m in range(WAY):
        h_copy(m).wait()


def forward(x, g, u, d):
    dma = pltpu.SemaphoreType.DMA
    return pl.pallas_call(
        forward_kernel,
        out_shape=(
            jax.ShapeDtypeStruct((2, 8, LANES, FF), BF),
            jax.ShapeDtypeStruct((2, 8, LANES, FF), BF),
            jax.ShapeDtypeStruct((2, 8, OWN, D), BF),
            jax.ShapeDtypeStruct((FF, T), BF),
            jax.ShapeDtypeStruct((D, T), BF),
            jax.ShapeDtypeStruct((T, D), BF),
        ),
        in_specs=[ANY] * WAY,
        out_specs=(ANY,) * 6,
        scratch_shapes=[
            pltpu.VMEM((T, D), BF),
            pltpu.VMEM((2, LANES, FF), BF),
            pltpu.VMEM((2, LANES, FF), BF),
            pltpu.VMEM((2, OWN, D), BF),
            pltpu.VMEM((D, FF), BF),
            pltpu.VMEM((D, FF), BF),
            pltpu.VMEM((FF, D), BF),
            pltpu.VMEM((T, FF), BF),
            pltpu.VMEM((TM, D), BF),
            pltpu.VMEM((D, TM), BF),
            pltpu.VMEM((FF, TM), BF),
            *[dma((6, 2, 3))] * 2, *[dma((6, 2, 3, 3))] * 2, *[dma((6, WAY))] * 2,
            dma((6,)), dma((6,)), dma, dma((3, 8)), *[dma((WAY,))] * 3,
        ],
        compiler_params=pltpu.CompilerParams(collective_id=0, has_side_effects=True, vmem_limit_bytes=VMEM_LIMIT),
        cost_estimate=cost(3, 60_000_000),
        name="forward",
    )(x, g, u, d)


def hidden_kernel(number, want_hid, h, by_y, G, U, Dn, *rest):
    outs, (a_nat, wg, wu, wd, sems) = rest[:-5], rest[-5:]
    hid_ref, a_ref = outs[:2] if want_hid else (None, None)
    dg_ref, du_ref = outs[-2:]
    m = pl.program_id(0)

    def copies(j):
        part = pl.ds(*GROUPS[j])
        return (
            pltpu.make_async_copy(G.at[number, :, part], wg.at[:, part], sems.at[0, j]),
            pltpu.make_async_copy(U.at[number, :, part], wu.at[:, part], sems.at[1, j]),
            pltpu.make_async_copy(Dn.at[number, part, :], wd.at[part, :], sems.at[2, j]),
        )

    @pl.when(m == 0)
    def _():
        for j in range(len(GROUPS)):
            for copy in copies(j):
                copy.start()

    a = normed(h[...])
    a_nat[...] = a
    if want_hid:
        a_ref[...] = a.T
    for j, (first, count) in enumerate(GROUPS):

        @pl.when(m == 0)
        def _():
            for copy in copies(j):
                copy.wait()

        for start, size in CHUNKS:
            if not first <= start < first + count:
                continue
            part = pl.ds(start, size)
            gate, up = dot(a_nat[...], wg[:, part]), dot(a_nat[...], wu[:, part])
            by_hid = dot_bt(by_y[...], wd[part, :]).astype(BF).astype(F32)
            sig = jax.nn.sigmoid(gate)
            act = gate * sig
            if want_hid:
                hid_ref[part, :] = (act * up).astype(BF).T
            du_ref[:, part] = (by_hid * act).astype(BF)
            dg_ref[:, part] = (by_hid * up * (sig + act * (1.0 - sig))).astype(BF)


def hidden(number, want_hid, h, by_y, G, U, Dn):
    tile = pl.BlockSpec((TM, D), lambda m: (m, 0))
    wide = pl.BlockSpec((TM, FF), lambda m: (m, 0))
    wide_shape = jax.ShapeDtypeStruct((T, FF), BF)
    extra_specs = (pl.BlockSpec((FF, TM), lambda m: (0, m)), pl.BlockSpec((D, TM), lambda m: (0, m))) if want_hid else ()
    extra_shapes = (jax.ShapeDtypeStruct((FF, T), BF), jax.ShapeDtypeStruct((D, T), BF)) if want_hid else ()
    return pl.pallas_call(
        functools.partial(hidden_kernel, number, want_hid),
        grid=(T // TM,),
        out_shape=extra_shapes + (wide_shape, wide_shape),
        in_specs=[tile, tile, ANY, ANY, ANY],
        out_specs=extra_specs + (wide, wide),
        scratch_shapes=[
            pltpu.VMEM((TM, D), BF),
            pltpu.VMEM((D, FF), BF),
            pltpu.VMEM((D, FF), BF),
            pltpu.VMEM((FF, D), BF),
            pltpu.SemaphoreType.DMA((3, len(GROUPS))),
        ],
        compiler_params=pltpu.CompilerParams(vmem_limit_bytes=VMEM_LIMIT),
        cost_estimate=cost(3, 70_000_000),
        name=f"hidden_{number}",
    )(h, by_y, G.reshape(2, D, FF), U.reshape(2, D, FF), Dn.reshape(2, FF, D))


UNITS = (
    ((64, SIDE), "yxz", "zy"),
    ((48, SIDE), "zxy", "yz"),
    ((TILE, WIDE), "xyz", "zy"),
    ((TILE, WIDE), "xzy", "yz"),
    ((TILE, WIDE), "yxz", "zy"),
    ((TILE, WIDE), "xzy", "yz"),
    ((TILE, WIDE), "xyz", "zy"),
    ((TILE, WIDE), "zxy", "yz"),
    ((TILE, LANES), "xyz", "yz"),
)
KINDS = ((0, 1), (1, 1), (2, 6), (8, 1))


def gradients_kernel(number, aT, hidT, by_y, h, G, U, Dn, *rest):
    if number:
        dg, du, g_out, u_out, d_out, h_out = rest[:6]
        rest = rest[6:]
    else:
        g_out, u_out, d_out = rest[:3]
        rest = rest[3:]
    a, rhs, hid, send_d, send_e, send_u, send_t, wg, wu, *rest = rest
    bufs, (pair_s, pair_r, s, r, a_sem, rhs_sem, hid_sem, y_sem, out_sem, w_sem, more, own, *wd) = rest[:24], rest[24:]
    ri, si = lax.axis_index("r"), lax.axis_index("s")
    core = si % 2
    me = {"x": si // 2, "y": ri // WAY, "z": ri % WAY}

    def peer(axis, k):
        if axis == "x":
            return {"r": ri, "s": 2 * ((me["x"] + k) % WAY) + core}
        if axis == "y":
            return {"r": ((me["y"] + k) % WAY) * WAY + me["z"], "s": si}
        return {"r": me["y"] * WAY + (me["z"] + k) % WAY, "s": si}

    partner = {"r": ri, "s": si + 1 - 2 * core}
    barrier = pltpu.get_barrier_semaphore()
    for to in [peer(axis, k) for axis in "xyz" for k in NEAR_FIRST] + [partner]:
        pl.semaphore_signal(barrier, inc=1, device_id=to, device_id_type=MESH)
    pl.semaphore_wait(barrier, 10)

    def buffers(unit):
        for kind, (first, count) in enumerate(KINDS):
            if first <= unit < first + count:
                return [ref.at[unit - first] for ref in bufs[6 * kind : 6 * kind + 6]]

    def others(unit, stage):
        order = UNITS[unit][1]
        return [axis for axis in "xyz" if axis in order[stage:]]

    def cut(unit, stage, index, half=None):
        axis, index_of = UNITS[unit][1][stage], []
        for one in others(unit, stage):
            if one == axis:
                index_of.append(index)
            elif half is None:
                index_of.append(slice(None))
            else:
                index_of.append(pl.ds(2 * half, 2))
                half = None
        return tuple(index_of)

    def halves_of(RA, axis, index, half=None):
        part = slice(None) if half is None else pl.ds(2 * half, 2)
        if axis == "y":
            return RA.at[1 + index, part]
        return RA.at[pl.ds(1, WAY) if half is None else pl.ds(1 + 2 * half, 2), index]

    def copies(unit, step):
        P, R1, Q1, R2, Q2, RA = buffers(unit)
        order, gather = UNITS[unit][1:]
        made = []
        for k in NEAR_FIRST if step in (WAY, 5) else SIDES:
            back = k // 2
            if step < WAY:
                stage = step // 2
                axis, src, dst = order[stage], (P, Q1)[stage], (R1, R2)[stage]
                if step % 2:
                    src, dst = src.at[cut(unit, stage, (me[axis] + k) % WAY)], dst.at[back]
                else:
                    src, dst = src.at[cut(unit, stage, (me[axis] + 2) % WAY, back)], dst.at[2, pl.ds(2 * back, 2)]
            elif step == WAY:
                axis = order[2]
                src, dst = Q2.at[(me[axis] + k) % WAY], RA.at[0, k - 1]
            elif step == 5:
                axis = gather[0]
                src = dst = RA.at[1 + me["y"], me["z"]]
            elif step == 6:
                axis = gather[1]
                src = dst = halves_of(RA, axis, me[axis])
            else:
                axis = gather[1]
                src = dst = halves_of(RA, axis, (me[axis] + WAY - k) % WAY, back)
            made.append(pltpu.make_async_remote_copy(
                src_ref=src, dst_ref=dst, send_sem=s.at[unit, step, k - 1], recv_sem=r.at[unit, step, k - 1],
                device_id=peer(axis, k), device_id_type=MESH))
        return made

    def start(unit, step):
        for copy in copies(unit, step):
            copy.start()

    def wait(unit, step):
        for copy in copies(unit, step):
            copy.wait_recv()

    def out_copies(unit):
        RA = buffers(unit)[5]
        made = []
        if unit < 2:
            base, rows = SIDE * unit, UNITS[unit][0][0]
            for y in range(WAY):
                for z in range(WAY if unit == 0 else 3):
                    made.append((RA.at[1 + y, z], d_out.at[pl.ds(base + z * rows, rows), pl.ds(y * SIDE, SIDE)]))
        else:
            columns = pl.ds(*CHUNKS[unit - 2])
            for y in range(WAY):
                out = (g_out, u_out)[y // 2]
                made += [(RA.at[1 + y, z], out.at[pl.ds((y % 2) * 64 + z * TILE, TILE), columns]) for z in range(WAY)]
        return [pltpu.make_async_copy(src, dst, out_sem.at[unit, n]) for n, (src, dst) in enumerate(made)]

    def advance(unit, step):
        P, R1, Q1, R2, Q2, RA = buffers(unit)
        wait(unit, step)
        stage = step // 2
        order = UNITS[unit][1]

        def first(index):
            at = list(index)
            at.insert("xyz".index(order[0]), me[order[0]])
            return P[tuple(at)].astype(F32) + R1[(0, *index)].astype(F32) + R1[(1, *index)].astype(F32)

        if step in (0, 2):
            R, to = (R1, R2)[stage], (P, Q1)[stage]
            for k in SIDES:
                index = cut(unit, stage, (me[order[stage]] + k) % WAY, k // 2)
                own = first(index) if stage else P[index].astype(F32)
                to[index] = (own + R[2, pl.ds(2 * (k // 2), 2)].astype(F32)).astype(BF)
        elif step == 1:
            Q1[...] = first((slice(None), slice(None))).astype(BF)
        elif step in (3, WAY):
            every = slice(None) if step == 3 else me[order[2]]
            index = [every if axis == order[2] else me[axis] for axis in others(unit, 1)]
            mine = first(tuple(index)) + R2[0, every].astype(F32) + R2[1, every].astype(F32)
            if step == 3:
                Q2[...] = mine.astype(BF)
            else:
                for k in range(3):
                    mine += RA[0, k].astype(F32)
                RA[1 + me["y"], me["z"]] = mine.astype(BF)
        if step < 7:
            start(unit, step + 1)
        else:
            for copy in out_copies(unit):
                copy.start()

    after = (
        "a0b0", "cs", "b1c0", "dsa1b2", "a2b3c1d0", "esa3b4c2", "a4b5c3d1e0", "fsa5b6c4d2",
        "a6b7c5d3e1f0", "gsa7c6d4e2", "c7d5e3f1g0", "hsd6e4f2", "isd7e5f3g1h0", "e6f4g2i0e7f5g3h1i1f6g4h2i2f7g5h3i3g6h4i4g7h5i5h6i6h7i7",
    )

    def run(tick):
        what = after[tick]
        for letter, step in zip(what[::2], what[1::2]):
            unit = ord(letter) - ord("a")
            if step == "s":
                start(unit, 0)
            else:
                advance(unit, int(step))

    def parity(half):
        return core if half else 1 - core

    def hid_copy(j):
        block = 2 * (j % WAY) + jnp.where(j < WAY, 1 - core, core)
        rows = pl.ds(pl.multiple_of(block * OWN, TILE), OWN)
        return pltpu.make_async_copy(hidT.at[rows], hid.at[j % 2], hid_sem.at[j % 2])

    def y_copy(half):
        return pltpu.make_async_copy(by_y.at[:, pl.ds(half * WIDE, WIDE)], rhs.at[1, half], y_sem.at[half])

    def columns_of(n):
        if isinstance(n, int) and n == 6:
            return pl.ds(3072, LANES), pl.ds(0, LANES)
        return pl.ds(pl.multiple_of(n * WIDE, WIDE), WIDE), slice(None)

    def w_copies(n):
        columns, to = columns_of(n)
        made = [(W.at[number, :, columns], w.at[n % 2, :, to]) for W, w in ((G, wg), (U, wu))]
        if number:
            made += [(d.at[:, columns], rhs.at[n % 2, mat, :, to]) for mat, d in enumerate((dg, du))]
        else:
            made.append((Dn.at[number, columns, :], wd[0].at[n % 2, to, :]))
        return [pltpu.make_async_copy(src, dst, w_sem.at[n % 2, i]) for i, (src, dst) in enumerate(made)]

    def w_start(n):
        for copy in w_copies(n):
            copy.start()

    def w_wait(n):
        for copy in w_copies(n):
            copy.wait()

    def tile(t):
        return pl.ds(pl.multiple_of(t * TM, TM), TM)

    PA, PB = buffers(0)[0], buffers(1)[0]

    def pair_d(k, which):
        src, dst = ((send_d, PA), (send_e, PB))[which]
        return pltpu.make_async_remote_copy(
            src_ref=src.at[k % 2], dst_ref=dst.at[k], send_sem=pair_s.at[k, which], recv_sem=pair_r.at[k, which],
            device_id=partner, device_id_type=MESH)

    hid_copy(0).start()
    for half in range(2):
        y_copy(half).start()

    def a_copy(half, x):
        rows = pl.ds(pl.multiple_of((2 * x + parity(half)) * LANES, LANES), LANES)
        return pltpu.make_async_copy(aT.at[rows], a.at[half, pl.ds(x * LANES, LANES)], a_sem.at[half, x])

    for half in range(2):
        for x in range(WAY):
            a_copy(half, x).start()
    w_start(0)
    if number:
        more[...] = jnp.zeros_like(more)
    else:
        x_copy = pltpu.make_async_copy(h, more, rhs_sem)
        x_copy.start()
    send_e[:, :, pl.ds(3, 1)] = jnp.zeros((2, WAY, 1, 48, SIDE), BF)
    for half in range(2):
        y_copy(half).wait()

    def down_step(j, carry):
        hid_copy(j).wait()

        @pl.when(j < 7)
        def _():
            hid_copy(j + 1).start()

        k = j % WAY

        @pl.when((j == 2) | (j == 3))
        def _():
            pair_d(k - 2, 0).wait_send()
            pair_d(k - 2, 1).wait_send()

        for half in range(2):
            out = dot(hid[j % 2], rhs[1, half])
            upper = [out[:SIDE, SIDE * n : SIDE * n + SIDE].reshape(WAY, 64, SIDE) for n in range(2)]
            lower = [out[SIDE:, SIDE * n : SIDE * n + SIDE].reshape(3, 48, SIDE) for n in range(2)]
            if half == 0:

                @pl.when(j >= WAY)
                def _():
                    pair_d(k, 0).wait_recv()
                    pair_d(k, 1).wait_recv()

            for n in range(2):
                y = 2 * half + n

                @pl.when(j < WAY)
                def _():
                    send_d[k % 2, y] = upper[n].astype(BF)
                    send_e[k % 2, y, pl.ds(0, 3)] = lower[n].astype(BF)

                @pl.when(j >= WAY)
                def _():
                    PA[k, y] = (PA[k, y].astype(F32) + upper[n]).astype(BF)
                    PB[k, y, pl.ds(0, 3)] = (PB[k, y, pl.ds(0, 3)].astype(F32) + lower[n]).astype(BF)

        @pl.when(j < WAY)
        def _():
            pair_d(k, 0).start()
            pair_d(k, 1).start()

        return carry

    lax.fori_loop(0, 8, down_step, 0)
    for unit in range(2):
        start(unit, 0)
    for half in range(2):
        for x in range(WAY):
            a_copy(half, x).wait()

    def by_gate_up(n, size):
        w_wait(n)
        if not (isinstance(n, int) and n == 6):

            @pl.when(n < 5)
            def _():
                w_start(n + 1)

            @pl.when(n == 5)
            def _():
                w_start(6)

        def one(t, carry):
            part = pl.ds(0, size)
            gate, up = (dot(more[tile(t), :], w[n % 2, :, part]) for w in (wg, wu))
            down = wd[0].at[n % 2, part]
            by_hid = dot_bt(rhs[1, 0, tile(t), :], down[:, :WIDE]) + dot_bt(rhs[1, 1, tile(t), :], down[:, WIDE:])
            by_hid = by_hid.astype(BF).astype(F32)
            sig = jax.nn.sigmoid(gate)
            act = gate * sig
            rhs[0, 1, tile(t), part] = (by_hid * act).astype(BF)
            rhs[0, 0, tile(t), part] = (by_hid * up * (sig + act * (1.0 - sig))).astype(BF)
            return carry

        lax.fori_loop(0, T // TM, one, 0)

    def by_input(n, size):
        part = pl.ds(0, size)

        def one(t, carry):
            for half in range(2):
                to = pl.ds(WIDE * half, WIDE)
                gate, up = (dot_bt(rhs[n % 2, mat, tile(t), part], w[n % 2, to, part]) for mat, w in enumerate((wg, wu)))
                more[tile(t), to] += gate + up
            return carry

        lax.fori_loop(0, T // TM, one, 0)

    if number:
        w_start(1)
    else:
        x_copy.wait()

        def norm(t, carry):
            more[tile(t), :] = normed(more[tile(t), :])
            return carry

        lax.fori_loop(0, T // TM, norm, 0)
        by_gate_up(0, WIDE)

    def gate_up(send, rights, pair, kept, columns):
        for mat in range(2):
            send[:, pl.ds(2 * mat, 2)] = dot(a[0], rights(mat)).astype(BF).reshape(WAY, 2, WAY, TILE, columns)
        pair.start()
        for mat in range(2):
            kept[:, pl.ds(2 * mat, 2)] = dot(a[1], rights(mat)).reshape(WAY, 2, WAY, TILE, columns)

    def pair_sum(P, pair, kept):
        pair.wait_recv()
        for x in range(WAY):
            P[x] = (P[x].astype(F32) + kept[x]).astype(BF)

    def pair_u(n):
        return pltpu.make_async_remote_copy(
            src_ref=send_u.at[n % 2], dst_ref=bufs[12].at[n], send_sem=pair_s.at[WAY + n, 0], recv_sem=pair_r.at[WAY + n, 0],
            device_id=partner, device_id_type=MESH)

    pair_t = pltpu.make_async_remote_copy(
        src_ref=send_t, dst_ref=buffers(8)[0], send_sem=pair_s.at[10, 0], recv_sem=pair_r.at[10, 0],
        device_id=partner, device_id_type=MESH)

    def chunk_step(n, carry):
        if number:
            w_wait(n)

        @pl.when(n >= 2)
        def _():
            pair_u(n - 2).wait_send()

        slot = n % 2 if number else 0
        gate_up(send_u.at[n % 2], lambda mat: rhs[slot, mat], pair_u(n), own, WIDE)
        for now in range(6):

            @pl.when(n == now)
            def _():
                run(2 * now)

        if number:
            by_input(n, WIDE)

            @pl.when(n < WAY)
            def _():
                w_start(n + 2)

            @pl.when(n == WAY)
            def _():
                w_start(6)

        else:

            @pl.when(n < 5)
            def _():
                by_gate_up(n + 1, WIDE)

            @pl.when(n == 5)
            def _():
                by_gate_up(6, LANES)

        pair_sum(bufs[12].at[n], pair_u(n), own)
        for now in range(6):

            @pl.when(n == now)
            def _():
                run(2 * now + 1)

        return carry

    lax.fori_loop(0, 6, chunk_step, 0)
    if number:
        w_wait(6)
    kept = own.at[:, :, :, :, pl.ds(0, LANES)]
    gate_up(send_t, lambda mat: rhs[0, mat, :, pl.ds(0, LANES)], pair_t, kept, LANES)
    pair_sum(buffers(8)[0], pair_t, kept)
    run(12)
    if number:
        by_input(6, LANES)

        def part_copies(slot, whole, back=False):
            made = []
            for half in range(2):
                refs = whole.at[:, pl.ds(half * WIDE, WIDE)], rhs.at[slot, half]
                made.append(pltpu.make_async_copy(*(refs[::-1] if back else refs), y_sem.at[half] if slot else rhs_sem.at[half]))
            return made

        loads = part_copies(0, h) + part_copies(1, by_y)
        for copy in loads:
            copy.start()
        for copy in loads:
            copy.wait()

        def one(t, carry):
            by_a = more[tile(t), :].astype(BF).astype(F32)
            by_a = [by_a[:, :WIDE], by_a[:, WIDE:]]
            wide = [rhs[0, half, tile(t), :].astype(F32) for half in range(2)]
            scale = lax.rsqrt(sum(jnp.sum(w * w, -1, keepdims=True) for w in wide) / D + 1e-6)
            along = sum(jnp.sum(b * w, -1, keepdims=True) for b, w in zip(by_a, wide)) / D
            for half in range(2):
                by_h = (by_a[half] * scale - wide[half] * (scale * scale * scale * along)).astype(BF)
                rhs[0, half, tile(t), :] = (rhs[1, half, tile(t), :].astype(F32) + by_h.astype(F32)).astype(BF)
            return carry

        lax.fori_loop(0, T // TM, one, 0)
        stores = part_copies(0, h_out, back=True)
        for copy in stores:
            copy.start()
        for copy in stores:
            copy.wait()
    run(13)

    for k in (2, 3):
        for which in range(2):
            pair_d(k, which).wait_send()
    for n in (WAY, 5):
        pair_u(n).wait_send()
    pair_t.wait_send()
    for unit in range(len(UNITS)):
        for step in range(8):
            for copy in copies(unit, step):
                copy.wait_send()
        for copy in out_copies(unit):
            copy.wait()


def gradients(number, aT, hidT, by_y, h, G, U, Dn, *by_gate_up):
    dma = pltpu.SemaphoreType.DMA
    bufs = []
    for first, count in KINDS:
        shape = UNITS[first][0]
        for ways in ((WAY, WAY, WAY), (3, WAY, WAY), (WAY, WAY), (3, WAY), (WAY,), (5, WAY)):
            bufs.append(pltpu.VMEM((count, *ways, *shape), BF))
    outs = [(LANES, FF), (LANES, FF), (OWN, D)] + [(T, D)] * number
    return pl.pallas_call(
        functools.partial(gradients_kernel, number),
        out_shape=[jax.ShapeDtypeStruct(shape, BF) for shape in outs],
        in_specs=[ANY] * (9 if number else 7),
        out_specs=[ANY] * len(outs),
        scratch_shapes=[
            pltpu.VMEM((2, WIDE, T), BF),
            pltpu.VMEM((2, 2, T, WIDE), BF),
            pltpu.VMEM((2, OWN, T), BF),
            pltpu.VMEM((2, WAY, WAY, 64, SIDE), BF),
            pltpu.VMEM((2, WAY, WAY, 48, SIDE), BF),
            pltpu.VMEM((2, WAY, WAY, WAY, TILE, WIDE), BF),
            pltpu.VMEM((WAY, WAY, WAY, TILE, LANES), BF),
            pltpu.VMEM((2, D, WIDE), BF),
            pltpu.VMEM((2, D, WIDE), BF),
            *bufs,
            *[dma((11, 2))] * 2, *[dma((9, 8, 3))] * 2, dma((2, WAY)), dma((2,)) if number else dma,
            dma((2,)), dma((2,)), dma((9, TILE)), dma((2, WAY)), pltpu.VMEM((T, D), F32 if number else BF),
            pltpu.VMEM((WAY, WAY, WAY, TILE, WIDE), F32),
            *([] if number else [pltpu.VMEM((2, WIDE, D), BF)]),
        ],
        compiler_params=pltpu.CompilerParams(collective_id=1 + number, has_side_effects=True, vmem_limit_bytes=VMEM_LIMIT),
        cost_estimate=cost(5 if number else 6, 60_000_000),
        name=f"gradients_{number}",
    )(aT, hidT, by_y, h, G.reshape(2, D, FF), U.reshape(2, D, FF), Dn.reshape(2, FF, D), *by_gate_up)


def adamw(w, m, v, g):
    m = 0.9 * m + 0.1 * g
    v = 0.95 * v + 0.05 * g * g
    step = m * lax.rsqrt(v + 1e-8) + 0.1 * w
    return (w - 0.02 * step).astype(BF), m, v


def solution(mesh):
    def step(x, dy, *arrays):
        weights, m, v = (arrays[i : i + 3] for i in (0, 3, 6))
        x, dy = x[0], dy[0]
        G, U, Dn, hid0, a0, h1 = forward(x, *weights)
        hid1, a1, dg1, du1 = hidden(1, True, h1, dy, G, U, Dn)
        *one, by_h1 = gradients(1, a1, hid1, dy, h1, G, U, Dn, dg1, du1)
        zero = gradients(0, a0, hid0, by_h1, x, G, U, Dn)
        summed = [jnp.stack(pair).astype(F32) for pair in zip(zero, one)]
        new = [adamw(w.astype(F32), m, v, g) for w, m, v, g in zip(weights, m, v, summed)]
        return tuple(one[which] for which in range(3) for one in new)

    states, cut = P(("rep", "r", "s")), P(None, "s")
    return jax.shard_map(
        step,
        mesh=mesh,
        in_specs=(states, states) + (cut,) * 9,
        out_specs=(P("rep", "s"),) * 9,
        check_vma=False,
    )
```
